512 devices in a mesh: lat: 16 (over y_lo, z), lon: 32 (over y_hi, x, core).
Axes of the slice: x: 4, y: 8 (y_hi: 4, y_lo: 2; y = y_hi * 2 + y_lo), z: 8, core: 2. Of those that a mesh axis runs over, the one named last changes fastest.
Arguments:
- state_grid: bfloat16 [96, 2688, 192], P('lat', 'lon'), may hold values from -6 to 6
- norm_gain: float32 [192], replicated, may hold values from 0.1 to 1.9
- w_qkv: bfloat16 [192, 576], replicated, may hold values from -0.4375 to 0.4375
- w_proj: bfloat16 [192, 192], replicated, may hold values from -1.25 to 1.25
- bias_table: float32 [8, 6, 253], replicated, may hold values from -6 to 300
- window_kind: int32 [16, 224], replicated, may hold values from 0 to 7
- cotangent: bfloat16 [96, 2688, 192], P('lat', 'lon'), may hold values from -6 to 6
Outputs:
- out_field: bfloat16 [96, 2688, 192], P('lat', 'lon')
- d_field: bfloat16 [96, 2688, 192], P('lat', 'lon')
- qkv_grad: float32 [192, 576], replicated
- proj_grad: float32 [192, 192], replicated
- table_grad: float32 [8, 6, 253], replicated
- gain_grad: float32 [192], replicated
The draws below stay inside these ranges and needn't reach their ends.
All inputs are finite; a program needn't handle non-finite values.
Results may differ from the reference program's by a relative error of at most 0.009.
Values may be sent and summed in bfloat16 or wider, within the bound.
No kernel may reach another device: no remote copies, remote signals or barrier semaphores. Data moves between devices by JAX's collectives and lax.ppermute only.
A program may use at most 64 MiB of HBM per device.

```python
import jax
import jax.numpy as jnp
from jax import lax

D = 192
HEADS = 6
WIN_LAT = 6
WIN_LON = 12
KINDS = 8
NLAT = 96
NLON = 2688
BANDS = 16
SECTORS = 224
REL = 253


def draw_bias_table(key, part):
    ground_key = jax.random.fold_in(key, 11)
    dims_all = (KINDS, HEADS, REL)
    return jnp.clip(jax.random.normal(ground_key, dims_all, jnp.float32), -6.0, 6.0)


def touch_ends(drawn, stream_key, least, largest):
    longest = drawn.shape.index(max(drawn.shape))
    spots = []
    for shift in (0, 1):
        where = [jax.random.randint(jax.random.fold_in(stream_key, axis), (), 0, length) for axis, length in enumerate(drawn.shape)]
        where[longest] = (where[longest] + shift) % drawn.shape[longest]
        spots.append(tuple(where))
    return drawn.at[spots[0]].set(least).at[spots[1]].set(largest)


def level_of(key, shape, split, least, high):
    level = 1.0
    for dim, parts in split:
        steps = jax.random.uniform(jax.random.fold_in(jax.random.fold_in(key, 6), dim), (parts,), jnp.float32, least / len(split), high / len(split))
        level = level * jnp.repeat(jnp.exp(steps), shape[dim] // parts).reshape((-1,) + (1,) * (len(shape) - 1 - dim))
    return level


def normal_values(key, shape, deviation, bound, cuts=(), held_as=jnp.bfloat16):
    array = deviation * jax.random.normal(key, shape, jnp.float32)
    if cuts:
        array = array * level_of(key, shape, cuts, -0.22, 0.18)
    return jnp.clip(array, -bound, bound).astype(held_as)


def setup_inputs(seed: int = 0) -> dict:
    arg_keys = jax.random.split(jax.random.key(seed), 8)
    return {
        "state_grid": normal_values(arg_keys[0], (NLAT, NLON, D), 1.0, 6.0, ((0, 16), (1, 32))),
        "norm_gain": jnp.clip(1.0 + 0.18 * jax.random.normal(arg_keys[1], (D,), jnp.float32), 0.1, 1.9),
        "w_qkv": normal_values(arg_keys[2], (D, 3 * D), D ** -0.5, 0.4375),
        "w_proj": normal_values(arg_keys[3], (D, D), (D // 8) ** -0.5, 1.25),
        "bias_table": draw_bias_table(jax.random.fold_in(arg_keys[7], 71), 0),
        "window_kind": touch_ends(jax.random.randint(arg_keys[5], (BANDS, SECTORS), 0, KINDS), jax.random.fold_in(arg_keys[5], 1), 0, KINDS - 1).astype(jnp.int32),
        "cotangent": normal_values(arg_keys[6], (NLAT, NLON, D), 1.0, 6.0, ((0, 16), (1, 32))),
    }


norm_eps = 1e-05
clip_eps = 1e-06
clip_level = 1.0
masked_score = -1e+30
highest = lax.Precision.HIGHEST

def widen(array_in):
    return array_in.astype(jnp.float32)

def relation_onehot(win_lat, win_lon):
    position = jnp.arange(win_lat * win_lon, dtype=jnp.int32)
    row_of = position // win_lon
    column = position % win_lon
    offset = (row_of[:, None] - row_of[None, :] + win_lat - 1) * (2 * win_lon - 1) + (column[:, None] - column[None, :] + win_lon - 1)
    extent = (2 * win_lat - 1) * (2 * win_lon - 1)
    return (offset.reshape(-1)[:, None] == jnp.arange(extent, dtype=jnp.int32)[None, :]).astype(jnp.float32)

def to_windows(source, win_lat, win_lon):
    rows_all, cols_all, channels = source.shape
    source = source.reshape(rows_all // win_lat, win_lat, cols_all // win_lon, win_lon, channels)
    return source.transpose(0, 2, 1, 3, 4).reshape(-1, win_lat * win_lon, channels)

def from_windows(windows, rows_all, cols_all, win_lat, win_lon):
    channels = windows.shape[-1]
    source = windows.reshape(rows_all // win_lat, cols_all // win_lon, win_lat, win_lon, channels)
    return source.transpose(0, 2, 1, 3, 4).reshape(rows_all, cols_all, channels)

def window_bias(bias_table, kinds_flat, onehot_rel, positions):
    kind_count, heads_n, extent = bias_table.shape
    spread = jnp.dot(bias_table.reshape(kind_count * heads_n, extent), onehot_rel.T, precision=highest, preferred_element_type=jnp.float32)
    kind_onehot = (kinds_flat[:, None] == jnp.arange(kind_count, dtype=jnp.int32)[None, :]).astype(jnp.float32)
    per_window = jnp.dot(kind_onehot, spread.reshape(kind_count, heads_n * positions * positions), precision=highest, preferred_element_type=jnp.float32)
    return (per_window.reshape(-1, heads_n, positions, positions), kind_onehot)

def attend_forward(x_windows, norm_gain, w_qkv, w_proj, bias_win, allowed):
    count, positions, channels = x_windows.shape
    head_size = channels // HEADS
    inv_sqrt = head_size ** (-0.5)
    flat_rows = x_windows.reshape(-1, channels).astype(jnp.float32)
    centre = flat_rows - lax.optimization_barrier(jnp.mean(flat_rows, axis=-1, keepdims=True))
    inverse = lax.rsqrt(lax.optimization_barrier(jnp.mean(centre * centre, axis=-1, keepdims=True)) + norm_eps)
    unit_rows = centre * inverse
    normed = (unit_rows * norm_gain).astype(jnp.bfloat16)
    qkv_rows = jnp.dot(normed, w_qkv, preferred_element_type=jnp.float32).astype(jnp.bfloat16)
    parts_qkv = qkv_rows.reshape(count, positions, 3, HEADS, head_size)
    queries = parts_qkv[:, :, 0]
    keys_in = parts_qkv[:, :, 1]
    values_in = parts_qkv[:, :, 2]
    scores = jnp.einsum('wihd,wjhd->whij', widen(queries), widen(keys_in), precision=highest) * inv_sqrt + bias_win
    scores = jnp.where(allowed, scores, masked_score)
    soft_probs = jax.nn.softmax(scores, axis=-1)
    probs_low = soft_probs.astype(jnp.bfloat16)
    mixed_rows = jnp.einsum('whij,wjhd->wihd', widen(probs_low), widen(values_in), precision=highest).astype(jnp.bfloat16).reshape(-1, channels)
    branch = jnp.dot(mixed_rows, w_proj, preferred_element_type=jnp.float32).astype(jnp.bfloat16)
    saved = (normed, unit_rows, inverse, queries, keys_in, values_in, soft_probs, probs_low, mixed_rows)
    return (saved, branch)

def attend_backward(saved, g_windows, keep_win, w_qkv, w_proj, norm_gain, kind_onehot, onehot_rel, table_dims):
    normed, unit_rows, inverse, queries, keys_in, values_in, soft_probs, probs_low, mixed_rows = saved
    count, heads_n, positions = (soft_probs.shape[0], soft_probs.shape[1], soft_probs.shape[2])
    channels = normed.shape[1]
    head_size = channels // heads_n
    inv_sqrt = head_size ** (-0.5)
    flat_g = g_windows.reshape(-1, channels)
    keep_rows = keep_win.reshape(-1, 1)
    keep_low = keep_rows.astype(jnp.bfloat16)
    grad_proj = jnp.dot((mixed_rows * keep_low).T, flat_g, preferred_element_type=jnp.float32)
    d_mixed = jnp.dot(flat_g, w_proj.T, preferred_element_type=jnp.float32).astype(jnp.bfloat16)
    d_mixed = d_mixed.reshape(count, positions, heads_n, head_size)
    d_probs = jnp.einsum('wihd,wjhd->whij', widen(d_mixed), widen(values_in), precision=highest)
    d_values = jnp.einsum('whij,wihd->wjhd', widen(probs_low), widen(d_mixed), precision=highest).astype(jnp.bfloat16)
    d_scores = soft_probs * (d_probs - lax.optimization_barrier(jnp.sum(soft_probs * d_probs, axis=-1, keepdims=True)))
    d_scores_low = d_scores.astype(jnp.bfloat16)
    d_queries = (jnp.einsum('whij,wjhd->wihd', widen(d_scores_low), widen(keys_in), precision=highest) * inv_sqrt).astype(jnp.bfloat16)
    d_keys = (jnp.einsum('whij,wihd->wjhd', widen(d_scores_low), widen(queries), precision=highest) * inv_sqrt).astype(jnp.bfloat16)
    d_qkv = jnp.stack([d_queries, d_keys, d_values], axis=2).reshape(-1, 3 * channels)
    grad_qkv = jnp.dot((normed * keep_low).T, d_qkv, preferred_element_type=jnp.float32)
    d_normed = jnp.dot(d_qkv, w_qkv.T, preferred_element_type=jnp.float32)
    grad_gain = lax.optimization_barrier(jnp.sum(d_normed * unit_rows * keep_rows, axis=0))
    d_unit = d_normed * norm_gain
    d_path = inverse * (d_unit - lax.optimization_barrier(jnp.mean(d_unit, axis=-1, keepdims=True)) - unit_rows * lax.optimization_barrier(jnp.mean(d_unit * unit_rows, axis=-1, keepdims=True)))
    d_path = d_path.astype(jnp.bfloat16)
    query_keep = keep_win.reshape(count, 1, positions, 1)
    by_kind = jnp.dot(kind_onehot.T, (d_scores * query_keep).reshape(count, -1), precision=highest, preferred_element_type=jnp.float32)
    grad_table = jnp.dot(by_kind.reshape(-1, positions * positions), onehot_rel, precision=highest, preferred_element_type=jnp.float32)
    return (d_path, (grad_qkv, grad_proj, grad_table.reshape(table_dims), grad_gain))

def clip_rms(gradient):
    return gradient * jnp.minimum(1.0, clip_level * lax.rsqrt(jnp.mean(gradient * gradient) + clip_eps))

def reference(state_grid, norm_gain, w_qkv, w_proj, bias_table, window_kind, cotangent):
    rows_all, cols_all, channels = state_grid.shape
    half_lat = WIN_LAT // 2
    half_lon = WIN_LON // 2
    positions = WIN_LAT * WIN_LON
    onehot_rel = relation_onehot(WIN_LAT, WIN_LON)
    rolled_x = jnp.roll(state_grid, (-half_lat, -half_lon), axis=(0, 1))
    rolled_g = jnp.roll(cotangent, (-half_lat, -half_lon), axis=(0, 1))
    stacked_x = rolled_x.reshape(BANDS, WIN_LAT, cols_all, channels)
    stacked_g = rolled_g.reshape(BANDS, WIN_LAT, cols_all, channels)
    row_index = jnp.arange(rows_all, dtype=jnp.int32)
    labels_all = (((row_index + half_lat) % rows_all + half_lat) // WIN_LAT).reshape(BANDS, WIN_LAT)

    def band_step(running, slab_in):
        band_x, band_g, band_kinds, band_labels = slab_in
        label_grid = jnp.broadcast_to(band_labels[:, None, None], (WIN_LAT, cols_all, 1))
        label_win = to_windows(label_grid, WIN_LAT, WIN_LON)[:, :, 0]
        allowed = (label_win[:, :, None] == label_win[:, None, :])[:, None]
        bias_win, kind_onehot = window_bias(bias_table, band_kinds, onehot_rel, positions)
        saved, branch = attend_forward(to_windows(band_x, WIN_LAT, WIN_LON), norm_gain, w_qkv, w_proj, bias_win, allowed)
        keep_win = jnp.ones(label_win.shape, jnp.float32)
        g_windows = to_windows(band_g, WIN_LAT, WIN_LON)
        d_path, grads = attend_backward(saved, g_windows, keep_win, w_qkv, w_proj, norm_gain, kind_onehot, onehot_rel, bias_table.shape)
        running = tuple((earlier + gradient for earlier, gradient in zip(running, grads)))
        branch_band = from_windows(branch.reshape(-1, positions, channels), WIN_LAT, cols_all, WIN_LAT, WIN_LON)
        path_band = from_windows(d_path.reshape(-1, positions, channels), WIN_LAT, cols_all, WIN_LAT, WIN_LON)
        return (running, (branch_band, path_band))
    zeros_init = (jnp.zeros((channels, 3 * channels), jnp.float32), jnp.zeros((channels, channels), jnp.float32), jnp.zeros(bias_table.shape, jnp.float32), jnp.zeros((channels,), jnp.float32))
    running, (branch_all, path_all) = lax.scan(band_step, zeros_init, (stacked_x, stacked_g, window_kind, labels_all))
    branch_all = jnp.roll(branch_all.reshape(rows_all, cols_all, channels), (half_lat, half_lon), axis=(0, 1))
    path_all = jnp.roll(path_all.reshape(rows_all, cols_all, channels), (half_lat, half_lon), axis=(0, 1))
    out_field = (state_grid.astype(jnp.float32) + branch_all.astype(jnp.float32)).astype(jnp.bfloat16)
    d_field = (cotangent.astype(jnp.float32) + path_all.astype(jnp.float32)).astype(jnp.bfloat16)
    return (out_field, d_field, clip_rms(running[0]), clip_rms(running[1]), clip_rms(running[2]), clip_rms(running[3]))
```

```python
import functools
import jax
import jax.numpy as jnp
from jax import lax
from jax.experimental import pallas as pl
from jax.experimental.pallas import tpu as pltpu
from jax.sharding import PartitionSpec as P

HEADS = 6
WIN_LAT = 6
WIN_LON = 12
HEAD = 32
D = 192
PITCH = 16
TOK = WIN_LAT * PITCH
LANES = 128
SPAN = 256
norm_eps = 1e-05
clip_eps = 1e-06
masked = -1e30
highest = lax.Precision.HIGHEST
f32 = jnp.float32
bf16 = jnp.bfloat16

NT = (((1,), (1,)), ((), ()))
TN = (((0,), (0,)), ((), ()))


def nt(a, b, **kw):
    return lax.dot_general(a, b, NT, preferred_element_type=f32, **kw)


def tn(a, b, **kw):
    return lax.dot_general(a, b, TN, preferred_element_type=f32, **kw)


def nn(a, b, **kw):
    return jnp.dot(a, b, preferred_element_type=f32, **kw)


def iota(shape, dim):
    return lax.broadcasted_iota(jnp.int32, shape, dim)


def base_pattern():
    p = iota((SPAN, SPAN), 0)
    lane = iota((SPAN, SPAN), 1)
    d = lane // PITCH
    c = lane % PITCH
    hit = (p == (2 * WIN_LAT - 2 - d) * (2 * WIN_LON - 1) - c + WIN_LON - 1) & (c < WIN_LON) & (d < 2 * WIN_LAT - 1)
    return hit.astype(f32)


def kernel(windows, meta_ref, s_ref, g_ref, up_ref, rt_ref, cr_ref, gain_ref, wqkv_ref, wproj_ref, table_ref,
           both_ref, gq_ref, gp_ref, gt_ref, gg_ref,
           xs, gs, tilt, span, bias, un, nm, inv, q_s, k_s, v_s, dm_s, mix, dq_s, dk_s, dv_s, fold):
    half_lat = WIN_LAT // 2
    half_lon = WIN_LON // 2
    own = windows * WIN_LON - half_lon
    kinds = table_ref.shape[0] // HEADS

    for c in range(PITCH):
        moved = table_ref[...] if c == 0 else pltpu.roll(table_ref[...], SPAN - c, axis=1)
        for half in range(2):
            tilt[half, pl.ds(c, kinds * HEADS, stride=PITCH), :] = moved[:, half * LANES:(half + 1) * LANES]
    pattern = base_pattern()
    span[...] = nn(jnp.concatenate([tilt[0], tilt[1]], axis=1), pattern, precision=highest)
    slot = iota((PITCH, LANES), 1)
    open_slot = (slot % PITCH < WIN_LON) & (slot < TOK)
    split = meta_ref[windows] > 0

    def spread(n, carry):
        wide = span[pl.ds(pl.multiple_of(n * PITCH, PITCH), PITCH), :]
        for r in range(WIN_LAT):
            off = (WIN_LAT - 1 - r) * PITCH
            part = wide if off == 0 else pltpu.roll(wide, SPAN - off, axis=1)
            other = (slot < half_lat * PITCH) if r >= half_lat else (slot >= half_lat * PITCH)
            ok = open_slot & jnp.logical_not(split & other)
            bias[n // HEADS, pl.ds(pl.multiple_of((n % HEADS) * TOK + r * PITCH, PITCH), PITCH), :] = jnp.where(ok, part[:, :LANES], masked)
        return carry

    lax.fori_loop(0, kinds * HEADS, spread, 0)
    fold[...] = jnp.zeros_like(fold)

    xs[...] = jnp.zeros_like(xs)
    gs[...] = jnp.zeros_like(gs)
    for w in range(windows):
        for r in range(WIN_LAT):
            at = w * TOK + r * PITCH
            start = half_lon + w * WIN_LON
            inside = WIN_LON if w < windows - 1 else half_lon
            for dst, src, lo in ((xs, s_ref, 0), (gs, g_ref, D)):
                if r < half_lat:
                    dst[at:at + inside, :] = src[r + half_lat, start:start + inside, :]
                    if inside < WIN_LON:
                        dst[at + inside:at + WIN_LON, :] = rt_ref[r, :, lo:lo + D]
                else:
                    dst[at:at + inside, :] = up_ref[r - half_lat, start:start + inside, lo:lo + D]
                    if inside < WIN_LON:
                        dst[at + inside:at + WIN_LON, :] = cr_ref[r - half_lat, :, lo:lo + D]

    gain = gain_ref[...]
    x = xs[...].astype(f32)
    centre = x - jnp.mean(x, axis=-1, keepdims=True)
    inverse = lax.rsqrt(jnp.mean(centre * centre, axis=-1, keepdims=True) + norm_eps)
    unit = centre * inverse
    un[...] = unit
    inv[...] = inverse
    normed = (unit * gain).astype(bf16)
    nm[...] = normed
    wq, wk, wv = (wqkv_ref[:, i * D:(i + 1) * D] for i in range(3))
    q_s[...] = nn(normed, wq).astype(bf16)
    k_s[...] = nn(normed, wk).astype(bf16)
    v_s[...] = nn(normed, wv).astype(bf16)
    dm_s[...] = nt(gs[...], wproj_ref[...]).astype(bf16)

    scale = HEAD ** (-0.5)
    head_of = iota((TOK, D), 1) // HEAD
    pads = jnp.zeros((LANES - TOK, D), bf16)

    def by_head(a):
        zero = jnp.zeros_like(a)
        return [jnp.where(head_of == h, a, zero) for h in range(HEADS)]

    def window(w, carry):
        rows = pl.ds(pl.multiple_of(w * TOK, TOK), TOK)
        kind = meta_ref[w]
        q, k, v, dm = q_s[rows, :], k_s[rows, :], v_s[rows, :], dm_s[rows, :]
        q_heads = jnp.concatenate(by_head(q), axis=0)
        dm_heads = jnp.concatenate(by_head(dm), axis=0)
        k_pad = jnp.concatenate([k, pads], axis=0)
        v_pad = jnp.concatenate([v, pads], axis=0)
        scores = nt(q_heads, k_pad) * scale + bias[kind]
        top = jnp.max(scores, axis=-1, keepdims=True)
        raised = jnp.exp(scores - top)
        probs = raised * (1.0 / jnp.sum(raised, axis=-1, keepdims=True))
        probs_low = probs.astype(bf16)
        d_probs = nt(dm_heads, v_pad)
        d_scores = probs * (d_probs - jnp.sum(probs * d_probs, axis=-1, keepdims=True))
        low = d_scores.astype(bf16)
        side = lambda a: jnp.concatenate([a[h * TOK:(h + 1) * TOK] for h in range(HEADS)], axis=1)
        tall = lambda a: jnp.concatenate([b for part in by_head(a) for b in (part, pads)], axis=0)
        mix[rows, :] = nn(side(probs_low), tall(v)).astype(bf16)
        dq_s[rows, :] = (nn(side(low), tall(k)) * scale).astype(bf16)
        dv_s[rows, :] = tn(probs_low, dm_heads)[:TOK].astype(bf16)
        dk_s[rows, :] = (tn(low, q_heads) * scale)[:TOK].astype(bf16)
        lane = iota((PITCH, SPAN), 1)
        for h in range(HEADS):
            total = None
            for r in range(WIN_LAT):
                off = (WIN_LAT - 1 - r) * PITCH
                part = d_scores[h * TOK + r * PITCH:h * TOK + (r + 1) * PITCH]
                part = jnp.concatenate([part, jnp.zeros_like(part)], axis=1)
                if off:
                    part = pltpu.roll(part, off, axis=1)
                total = part if total is None else total + part
            fold[kind, h * PITCH:(h + 1) * PITCH, :] += total
        return carry

    lax.fori_loop(0, windows, window, 0)

    branch = nn(mix[...], wproj_ref[...]).astype(bf16)
    gp_ref[...] = tn(mix[...], gs[...])
    d_normed = nt(dq_s[...], wq) + nt(dk_s[...], wk) + nt(dv_s[...], wv)
    for i, d in enumerate((dq_s, dk_s, dv_s)):
        gq_ref[:, i * D:(i + 1) * D] = tn(nm[...], d[...])
    unit = un[...]
    gg_ref[...] = jnp.sum(d_normed * unit, axis=0, keepdims=True)
    d_unit = d_normed * gain
    path = inv[...] * (d_unit - jnp.mean(d_unit, axis=-1, keepdims=True) - unit * jnp.mean(d_unit * unit, axis=-1, keepdims=True))
    path = path.astype(bf16)
    for w in range(windows):
        for r in range(WIN_LAT):
            at = w * TOK + r * PITCH
            both_ref[r, w * WIN_LON:(w + 1) * WIN_LON, 0:D] = branch[at:at + WIN_LON]
            both_ref[r, w * WIN_LON:(w + 1) * WIN_LON, D:2 * D] = path[at:at + WIN_LON]

    back = nt(fold[...].reshape(kinds * HEADS * PITCH, SPAN), pattern, precision=highest)
    for half in range(2):
        tilt[half] = back[:, half * LANES:(half + 1) * LANES]
    total = None
    for c in range(WIN_LON):
        part = jnp.concatenate([tilt[half, pl.ds(c, kinds * HEADS, stride=PITCH), :] for half in range(2)], axis=1)
        if c:
            part = pltpu.roll(part, c, axis=1)
        total = part if total is None else total + part
    gt_ref[...] = total


def attend(meta, s, g, up, rt, cr, gain, w_qkv, w_proj, table):
    windows = s.shape[1] // WIN_LON
    n = windows * TOK
    vm = pl.BlockSpec(memory_space=pltpu.VMEM)
    kh = table.shape[0]
    return pl.pallas_call(
        functools.partial(kernel, windows),
        out_shape=(
            jax.ShapeDtypeStruct(s.shape[:2] + (2 * D,), bf16),
            jax.ShapeDtypeStruct((D, 3 * D), f32),
            jax.ShapeDtypeStruct((D, D), f32),
            jax.ShapeDtypeStruct((kh, SPAN), f32),
            jax.ShapeDtypeStruct((1, D), f32),
        ),
        in_specs=[pl.BlockSpec(memory_space=pltpu.SMEM)] + [vm] * 9,
        out_specs=(vm,) * 5,
        scratch_shapes=[
            pltpu.VMEM((n, D), bf16), pltpu.VMEM((n, D), bf16),
            pltpu.VMEM((2, kh * PITCH, LANES), f32), pltpu.VMEM((kh * PITCH, SPAN), f32),
            pltpu.VMEM((kh // HEADS, HEADS * TOK, LANES), f32),
            pltpu.VMEM((n, D), f32), pltpu.VMEM((n, D), bf16), pltpu.VMEM((n, 1), f32),
        ] + [pltpu.VMEM((n, D), bf16)] * 8 + [pltpu.VMEM((kh // HEADS, HEADS * PITCH, SPAN), f32)],
        cost_estimate=pl.CostEstimate(flops=2_000_000_000, bytes_accessed=4_000_000, transcendentals=500_000),
        name="attend",
    )(meta, s, g, up, rt, cr, gain, w_qkv, w_proj, table)


def shifted(value, axis, steps):
    count = lax.axis_size(axis)
    return lax.ppermute(value, axis, [(i, (i + steps) % count) for i in range(count)])


def clip_rms(gradient, count):
    return gradient * jnp.minimum(1.0, lax.rsqrt(jnp.sum(gradient * gradient) / count + clip_eps))


ROWS = 1280


def total_of(packed):
    sizes = [lax.axis_size(a) for a in ("lat", "lon")]
    part = packed
    for axis, n in zip(("lat", "lon"), sizes):
        part = part.reshape((n, -1) + part.shape[1:]) if part.shape[0] % n == 0 else part.reshape(n, -1)
        got = lax.all_to_all(part, axis, 0, 0, tiled=True)
        part = jnp.sum(got.astype(f32), axis=0).astype(bf16)
    for axis, n in zip(("lon", "lat"), sizes[::-1]):
        part = lax.all_to_all(jnp.broadcast_to(part[None], (n,) + part.shape), axis, 0, 0, tiled=True)
    return part.reshape(-1)


def on_device(state_grid, norm_gain, w_qkv, w_proj, bias_table, window_kind, cotangent):
    rows_dev, cols_dev, channels = state_grid.shape
    half_lat, half_lon = WIN_LAT // 2, WIN_LON // 2
    lat, lon = lax.axis_index("lat"), lax.axis_index("lon")
    windows = cols_dev // WIN_LON
    joint = jnp.concatenate([state_grid[:half_lat], cotangent[:half_lat]], axis=2)
    up = shifted(joint, "lat", -1)
    side = jnp.concatenate([state_grid[half_lat:, :half_lon], cotangent[half_lat:, :half_lon]], axis=2)
    side = shifted(jnp.concatenate([side, up[:, :half_lon]], axis=0), "lon", -1)
    kinds = lax.dynamic_slice(window_kind, (lat, lon * windows), (1, windows))[0]
    last = (lat == lax.axis_size("lat") - 1).astype(jnp.int32)
    meta = jnp.concatenate([kinds, last[None]])
    kind_count, heads, extent = bias_table.shape
    table = jnp.pad(bias_table.reshape(kind_count * heads, extent), ((0, 0), (0, SPAN - extent)))
    both, gq, gp, gt, gg = attend(
        meta, state_grid, cotangent, up, side[:half_lat], side[half_lat:], norm_gain.reshape(1, -1), w_qkv, w_proj, table
    )
    moved = shifted(both[:, -half_lon:], "lon", 1)
    placed = jnp.concatenate([moved, both[:, :-half_lon]], axis=1)
    lower = shifted(placed[half_lat:], "lat", 1)
    own = jnp.concatenate([lower, placed[:half_lat]], axis=0).astype(f32)
    out_field = (state_grid.astype(f32) + own[:, :, :channels]).astype(bf16)
    d_field = (cotangent.astype(f32) + own[:, :, channels:]).astype(bf16)
    pieces = [gq, gp, gt[:, :extent], gg]
    flat = jnp.concatenate([p.astype(bf16).ravel() for p in pieces])
    flat = jnp.pad(flat, (0, ROWS * LANES - flat.size))
    summed = total_of(flat.reshape(ROWS, LANES))
    outs, at = [], 0
    for p in pieces:
        size = 1
        for n in p.shape:
            size *= n
        outs.append(clip_rms(summed[at:at + size].astype(f32), size))
        at += size
    return (out_field, d_field, outs[0].reshape(w_qkv.shape), outs[1].reshape(w_proj.shape),
            outs[2].reshape(bias_table.shape), outs[3])


def solution(mesh):
    in_specs = (P("lat", "lon", None), P(), P(), P(), P(), P(), P("lat", "lon", None))
    out_specs = (P("lat", "lon", None), P("lat", "lon", None), P(), P(), P(), P())
    return jax.shard_map(on_device, mesh=mesh, in_specs=in_specs, out_specs=out_specs, check_vma=False)
```

```python
import functools
import jax
import jax.numpy as jnp
from jax import lax
from jax.experimental import pallas as pl
from jax.experimental.pallas import tpu as pltpu
from jax.sharding import Mesh, PartitionSpec as P

HEADS = 6
WIN_LAT = 6
WIN_LON = 12
HEAD = 32
D = 192
PITCH = 16
TOK = WIN_LAT * PITCH
LANES = 128
SPAN = 256
norm_eps = 1e-05
clip_eps = 1e-06
masked = -1e30
AT_TABLE = 6 * D
AT_GAIN = AT_TABLE + 96
ROWS = 1280
LAT = ("y_lo", "z_hi", "z_lo")
LON = ("y_hi", "x", "core")
PARTS = (2, 4, 2, 4, 4, 2)
SLICED = ("y_lo", "z_lo", "x", "core")
WHOLE = (("z_hi", "y_hi"),)
highest = lax.Precision.HIGHEST
f32 = jnp.float32
bf16 = jnp.bfloat16

NT = (((1,), (1,)), ((), ()))
TN = (((0,), (0,)), ((), ()))


def nt(a, b, **kw):
    return lax.dot_general(a, b, NT, preferred_element_type=f32, **kw)


def tn(a, b, **kw):
    return lax.dot_general(a, b, TN, preferred_element_type=f32, **kw)


def nn(a, b, **kw):
    return jnp.dot(a, b, preferred_element_type=f32, **kw)


def iota(shape, dim):
    return lax.broadcasted_iota(jnp.int32, shape, dim)


def base_pattern():
    p = iota((SPAN, SPAN), 0)
    lane = iota((SPAN, SPAN), 1)
    d = lane // PITCH
    c = lane % PITCH
    hit = (p == (2 * WIN_LAT - 2 - d) * (2 * WIN_LON - 1) - c + WIN_LON - 1) & (c < WIN_LON) & (d < 2 * WIN_LAT - 1)
    return hit.astype(f32)


def kernel(windows, meta_ref, s_ref, g_ref, up_ref, side_ref, gain_ref, wqkv_ref, wproj_ref, table_ref,
           both_ref, grads_ref,
           xs, gs, tab, tilt, span, bias, un, nm, inv, q_s, k_s, v_s, dm_s, mix, dq_s, dk_s, dv_s, fold):
    half_lat = WIN_LAT // 2
    half_lon = WIN_LON // 2
    kinds = table_ref.shape[0] // HEADS

    tab[...] = jnp.zeros_like(tab)
    tab[:, :table_ref.shape[1]] = table_ref[...]
    for c in range(PITCH):
        moved = tab[...] if c == 0 else pltpu.roll(tab[...], SPAN - c, axis=1)
        for half in range(2):
            tilt[half, pl.ds(c, kinds * HEADS, stride=PITCH), :] = moved[:, half * LANES:(half + 1) * LANES]
    pattern = base_pattern()
    span[...] = nn(jnp.concatenate([tilt[0], tilt[1]], axis=1), pattern, precision=highest)
    slot = iota((PITCH, LANES), 1)
    open_slot = (slot % PITCH < WIN_LON) & (slot < TOK)
    split = meta_ref[windows] > 0

    def spread(n, carry):
        wide = span[pl.ds(pl.multiple_of(n * PITCH, PITCH), PITCH), :]
        for r in range(WIN_LAT):
            off = (WIN_LAT - 1 - r) * PITCH
            part = wide if off == 0 else pltpu.roll(wide, SPAN - off, axis=1)
            other = (slot < half_lat * PITCH) if r >= half_lat else (slot >= half_lat * PITCH)
            ok = open_slot & jnp.logical_not(split & other)
            bias[n % kinds, pl.ds(pl.multiple_of((n // kinds) * TOK + r * PITCH, PITCH), PITCH), :] = jnp.where(ok, part[:, :LANES], masked)
        return carry

    lax.fori_loop(0, kinds * HEADS, spread, 0)
    fold[...] = jnp.zeros_like(fold)

    xs[...] = jnp.zeros_like(xs)
    gs[...] = jnp.zeros_like(gs)
    for w in range(windows):
        for r in range(WIN_LAT):
            at = w * TOK + r * PITCH
            start = half_lon + w * WIN_LON
            inside = WIN_LON if w < windows - 1 else half_lon
            for dst, src, lo in ((xs, s_ref, 0), (gs, g_ref, D)):
                if r < half_lat:
                    dst[at:at + inside, :] = src[r + half_lat, start:start + inside, :]
                    if inside < WIN_LON:
                        dst[at + inside:at + WIN_LON, :] = side_ref[r, :, lo:lo + D]
                else:
                    dst[at:at + inside, :] = up_ref[r - half_lat, start:start + inside, lo:lo + D]
                    if inside < WIN_LON:
                        dst[at + inside:at + WIN_LON, :] = side_ref[r, :, lo:lo + D]

    gain = gain_ref[...]
    x = xs[...].astype(f32)
    centre = x - jnp.mean(x, axis=-1, keepdims=True)
    inverse = lax.rsqrt(jnp.mean(centre * centre, axis=-1, keepdims=True) + norm_eps)
    unit = centre * inverse
    un[...] = unit
    inv[...] = inverse
    normed = (unit * gain).astype(bf16)
    nm[...] = normed
    wq, wk, wv = (wqkv_ref[:, i * D:(i + 1) * D] for i in range(3))
    q_s[...] = nn(normed, wq).astype(bf16)
    k_s[...] = nn(normed, wk).astype(bf16)
    v_s[...] = nn(normed, wv).astype(bf16)
    dm_s[...] = nt(gs[...], wproj_ref[...]).astype(bf16)

    scale = HEAD ** (-0.5)
    head_of = iota((TOK, D), 1) // HEAD
    pads = jnp.zeros((LANES - TOK, D), bf16)

    def by_head(a):
        zero = jnp.zeros_like(a)
        return [jnp.where(head_of == h, a, zero) for h in range(HEADS)]

    def window(w, carry):
        rows = pl.ds(pl.multiple_of(w * TOK, TOK), TOK)
        kind = meta_ref[w]
        q, k, v, dm = q_s[rows, :], k_s[rows, :], v_s[rows, :], dm_s[rows, :]
        q_heads = jnp.concatenate(by_head(q), axis=0)
        dm_heads = jnp.concatenate(by_head(dm), axis=0)
        k_pad = jnp.concatenate([k, pads], axis=0)
        v_pad = jnp.concatenate([v, pads], axis=0)
        scores = nt(q_heads, k_pad) * scale + bias[kind]
        top = jnp.max(scores, axis=-1, keepdims=True)
        raised = jnp.exp(scores - top)
        probs = raised * (1.0 / jnp.sum(raised, axis=-1, keepdims=True))
        probs_low = probs.astype(bf16)
        d_probs = nt(dm_heads, v_pad)
        d_scores = probs * (d_probs - jnp.sum(probs * d_probs, axis=-1, keepdims=True))
        low = d_scores.astype(bf16)
        side = lambda a: jnp.concatenate([a[h * TOK:(h + 1) * TOK] for h in range(HEADS)], axis=1)
        tall = lambda a: jnp.concatenate([b for part in by_head(a) for b in (part, pads)], axis=0)
        mix[rows, :] = nn(side(probs_low), tall(v)).astype(bf16)
        dq_s[rows, :] = (nn(side(low), tall(k)) * scale).astype(bf16)
        dv_s[rows, :] = tn(probs_low, dm_heads)[:TOK].astype(bf16)
        dk_s[rows, :] = (tn(low, q_heads) * scale)[:TOK].astype(bf16)
        for h in range(HEADS):
            total = None
            for r in range(WIN_LAT):
                off = (WIN_LAT - 1 - r) * PITCH
                part = d_scores[h * TOK + r * PITCH:h * TOK + (r + 1) * PITCH]
                part = jnp.concatenate([part, jnp.zeros_like(part)], axis=1)
                if off:
                    part = pltpu.roll(part, off, axis=1)
                total = part if total is None else total + part
            fold[pl.ds(pl.multiple_of((h * kinds + kind) * PITCH, PITCH), PITCH), :] += total
        return carry

    lax.fori_loop(0, windows, window, 0)

    branch = nn(mix[...], wproj_ref[...]).astype(bf16)
    gp = tn(mix[...], gs[...]).astype(bf16)
    d_normed = nt(dq_s[...], wq) + nt(dk_s[...], wk) + nt(dv_s[...], wv)
    gq = []
    for i, d in enumerate((dq_s, dk_s, dv_s)):
        gq.append(tn(nm[...], d[...]).astype(bf16))
    gq = jnp.concatenate(gq, axis=1)
    for b in range(4):
        grads_ref[b * D:(b + 1) * D, :] = gq[:, b * LANES:(b + 1) * LANES]
    grads_ref[4 * D:5 * D, :] = jnp.concatenate([gq[:, 4 * LANES:], gp[:, LANES:]], axis=1)
    grads_ref[5 * D:6 * D, :] = gp[:, :LANES]
    unit = un[...]
    gg = jnp.sum(d_normed * unit, axis=0, keepdims=True)
    gg = jnp.concatenate([gg[:, :LANES], jnp.concatenate([gg[:, LANES:], jnp.zeros((1, SPAN - D), f32)], axis=1), jnp.zeros((ROWS - AT_GAIN - 2, LANES), f32)], axis=0)
    grads_ref[AT_GAIN:, :] = gg.astype(bf16)
    d_unit = d_normed * gain
    path = inv[...] * (d_unit - jnp.mean(d_unit, axis=-1, keepdims=True) - unit * jnp.mean(d_unit * unit, axis=-1, keepdims=True))
    path = path.astype(bf16)
    for w in range(windows):
        for r in range(WIN_LAT):
            at = w * TOK + r * PITCH
            both_ref[r, w * WIN_LON:(w + 1) * WIN_LON, 0:D] = branch[at:at + WIN_LON]
            both_ref[r, w * WIN_LON:(w + 1) * WIN_LON, D:2 * D] = path[at:at + WIN_LON]

    back = nt(fold[...], pattern, precision=highest)
    for half in range(2):
        tilt[half] = back[:, half * LANES:(half + 1) * LANES]
    total = None
    for c in range(WIN_LON):
        part = jnp.concatenate([tilt[half, pl.ds(c, kinds * HEADS, stride=PITCH), :] for half in range(2)], axis=1)
        if c:
            part = pltpu.roll(part, c, axis=1)
        total = part if total is None else total + part
    for half in range(2):
        at = AT_TABLE + half * kinds * HEADS
        grads_ref[at:at + kinds * HEADS, :] = total[:, half * LANES:(half + 1) * LANES].astype(bf16)


def attend(meta, s, g, up, side, gain, w_qkv, w_proj, table):
    windows = s.shape[1] // WIN_LON
    n = windows * TOK
    vm = pl.BlockSpec(memory_space=pltpu.VMEM)
    kh = table.shape[0]
    return pl.pallas_call(
        functools.partial(kernel, windows),
        out_shape=(
            jax.ShapeDtypeStruct(s.shape[:2] + (2 * D,), bf16),
            jax.ShapeDtypeStruct((ROWS, LANES), bf16),
        ),
        in_specs=[pl.BlockSpec(memory_space=pltpu.SMEM)] + [vm] * 8,
        out_specs=(vm,) * 2,
        scratch_shapes=[
            pltpu.VMEM((n, D), bf16), pltpu.VMEM((n, D), bf16), pltpu.VMEM((kh, SPAN), f32),
            pltpu.VMEM((2, kh * PITCH, LANES), f32), pltpu.VMEM((kh * PITCH, SPAN), f32),
            pltpu.VMEM((kh // HEADS, HEADS * TOK, LANES), f32),
            pltpu.VMEM((n, D), f32), pltpu.VMEM((n, D), bf16), pltpu.VMEM((n, 1), f32),
        ] + [pltpu.VMEM((n, D), bf16)] * 8 + [pltpu.VMEM((kh * PITCH, SPAN), f32)],
        cost_estimate=pl.CostEstimate(flops=2_000_000_000, bytes_accessed=4_000_000, transcendentals=500_000),
        name="attend",
    )(meta, s, g, up, side, gain, w_qkv, w_proj, table)


def finish_kernel(grads_ref, gq_ref, gp_ref, gt_ref, gg_ref):
    def scale_of(parts, count):
        total = sum(jnp.sum(jnp.sum(p * p, axis=0, keepdims=True), axis=1, keepdims=True) for p in parts)
        return jnp.minimum(1.0, lax.rsqrt(total / count + clip_eps))

    kh = gt_ref.shape[0]
    wide = [grads_ref[b * D:(b + 1) * D, :].astype(f32) for b in range(4)]
    shared = grads_ref[4 * D:5 * D, :].astype(f32)
    low, high = shared[:, :LANES // 2], shared[:, LANES // 2:]
    first = grads_ref[5 * D:6 * D, :].astype(f32)
    by = scale_of(wide + [low], gq_ref.shape[0] * gq_ref.shape[1])
    for b in range(4):
        gq_ref[:, b * LANES:(b + 1) * LANES] = wide[b] * by
    gq_ref[:, 4 * LANES:] = low * by
    by = scale_of([first, high], gp_ref.shape[0] * gp_ref.shape[1])
    gp_ref[:, :LANES] = first * by
    gp_ref[:, LANES:] = high * by
    left = grads_ref[AT_TABLE:AT_TABLE + kh, :].astype(f32)
    right = grads_ref[AT_TABLE + kh:AT_TABLE + 2 * kh, :].astype(f32)
    by = scale_of([left, right], kh * gt_ref.shape[1])
    gt_ref[:, :LANES] = left * by
    gt_ref[:, LANES:] = (right * by)[:, :gt_ref.shape[1] - LANES]
    rows = grads_ref[AT_GAIN:AT_GAIN + 16, :].astype(f32)
    by = scale_of([rows], D)
    gg_ref[:, :LANES] = rows[0:1] * by
    gg_ref[:, LANES:] = (rows[1:2] * by)[:, :D - LANES]


def finish(grads, table_rows, extent):
    vm = pl.BlockSpec(memory_space=pltpu.VMEM)
    return pl.pallas_call(
        finish_kernel,
        out_shape=(
            jax.ShapeDtypeStruct((D, 3 * D), f32),
            jax.ShapeDtypeStruct((D, D), f32),
            jax.ShapeDtypeStruct((table_rows, extent), f32),
            jax.ShapeDtypeStruct((1, D), f32),
        ),
        in_specs=[vm],
        out_specs=(vm,) * 4,
        cost_estimate=pl.CostEstimate(flops=1_000_000, bytes_accessed=1_000_000, transcendentals=4),
        name="finish",
    )(grads)


def shifted(value, axis, steps):
    count = lax.axis_size(axis)
    return lax.ppermute(value, axis, [(i, (i + steps) % count) for i in range(count)])


def spread_sum(part, axes):
    n = lax.axis_size(axes)
    got = lax.all_to_all(part.reshape(n, -1, LANES), axes, 0, 0, tiled=True)
    return jnp.sum(got.astype(f32), axis=0).astype(bf16)


def collect(part, axes):
    n = lax.axis_size(axes)
    return lax.all_to_all(jnp.broadcast_to(part[None], (n,) + part.shape), axes, 0, 0, tiled=True)


def total_of(packed):
    part = spread_sum(packed, SLICED)
    for axes in WHOLE:
        part = jnp.sum(collect(part, axes).astype(f32), axis=0).astype(bf16)
    return collect(part, SLICED).reshape(-1, LANES)


def on_device(state_grid, norm_gain, w_qkv, w_proj, bias_table, window_kind, cotangent):
    rows_dev, cols_dev, channels = state_grid.shape
    half_lat, half_lon = WIN_LAT // 2, WIN_LON // 2
    lat, lon = lax.axis_index(LAT), lax.axis_index(LON)
    windows = cols_dev // WIN_LON
    joint = jnp.concatenate([state_grid[:half_lat], cotangent[:half_lat]], axis=2)
    up = shifted(joint, LAT, -1)
    side = jnp.concatenate([state_grid[half_lat:, :half_lon], cotangent[half_lat:, :half_lon]], axis=2)
    side = shifted(jnp.concatenate([side, up[:, :half_lon]], axis=0), LON, -1)
    kinds = lax.dynamic_slice(window_kind, (lat, lon * windows), (1, windows))[0]
    last = (lat == lax.axis_size(LAT) - 1).astype(jnp.int32)
    meta = jnp.concatenate([kinds, last[None]])
    kind_count, heads, extent = bias_table.shape
    table = bias_table.transpose(1, 0, 2).reshape(heads * kind_count, extent)
    both, packed = attend(meta, state_grid, cotangent, up, side, norm_gain.reshape(1, -1), w_qkv, w_proj, table)
    moved = shifted(both[:, -half_lon:], LON, 1)
    placed = jnp.concatenate([moved, both[:, :-half_lon]], axis=1)
    lower = shifted(placed[half_lat:], LAT, 1)
    own = jnp.concatenate([lower, placed[:half_lat]], axis=0).astype(f32)
    out_field = (state_grid.astype(f32) + own[:, :, :channels]).astype(bf16)
    d_field = (cotangent.astype(f32) + own[:, :, channels:]).astype(bf16)
    gq, gp, gt, gg = finish(total_of(packed), heads * kind_count, extent)
    gt = gt.reshape(heads, kind_count, extent).transpose(1, 0, 2)
    return (out_field, d_field, gq, gp, gt, gg.reshape(-1))


def solution(mesh):
    in_specs = (P(LAT, LON, None), P(), P(), P(), P(), P(), P(LAT, LON, None))
    out_specs = (P(LAT, LON, None), P(LAT, LON, None), P(), P(), P(), P())
    mesh = Mesh(mesh.devices.reshape(PARTS), LAT + LON)
    return jax.shard_map(on_device, mesh=mesh, in_specs=in_specs, out_specs=out_specs, check_vma=False)
```

```python
import functools
import jax
import jax.numpy as jnp
from jax import lax
from jax.experimental import pallas as pl
from jax.experimental.pallas import tpu as pltpu
from jax.sharding import Mesh, PartitionSpec as P

HEADS = 6
WIN_LAT = 6
WIN_LON = 12
HEAD = 32
D = 192
PITCH = 16
TOK = WIN_LAT * PITCH
LANES = 128
SPAN = 256
norm_eps = 1e-05
clip_eps = 1e-06
masked = -1e30
AT_TABLE = 6 * D
AT_GAIN = AT_TABLE + 96
ROWS = 1280
VM_ATTEND = 28
VM_FINISH = 8
LAT = ("y_lo", "z_hi", "z_lo")
LON = ("y_hi", "x", "core")
PARTS = (2, 4, 2, 4, 4, 2)
SLICED = ("y_lo", "z_lo", "x", "core")
WHOLE = (("z_hi", "y_hi"),)
highest = lax.Precision.HIGHEST
f32 = jnp.float32
bf16 = jnp.bfloat16

NT = (((1,), (1,)), ((), ()))
TN = (((0,), (0,)), ((), ()))


def nt(a, b, **kw):
    return lax.dot_general(a, b, NT, preferred_element_type=f32, **kw)


def tn(a, b, **kw):
    return lax.dot_general(a, b, TN, preferred_element_type=f32, **kw)


def nn(a, b, **kw):
    return jnp.dot(a, b, preferred_element_type=f32, **kw)


def iota(shape, dim):
    return lax.broadcasted_iota(jnp.int32, shape, dim)


def base_pattern():
    p = iota((SPAN, SPAN), 0)
    lane = iota((SPAN, SPAN), 1)
    d = lane // PITCH
    c = lane % PITCH
    hit = (p == (2 * WIN_LAT - 2 - d) * (2 * WIN_LON - 1) - c + WIN_LON - 1) & (c < WIN_LON) & (d < 2 * WIN_LAT - 1)
    return hit.astype(f32)


def kernel(windows, meta_ref, s_ref, g_ref, up_ref, side_ref, gain_ref, wqkv_ref, wproj_ref, table_ref,
           both_ref, grads_ref,
           xs, gs, tab, tilt, span, bias, un, nm, inv, q_s, k_s, v_s, dm_s, mix, dq_s, dk_s, dv_s, fold):
    half_lat = WIN_LAT // 2
    half_lon = WIN_LON // 2
    kinds = table_ref.shape[0] // HEADS

    tab[...] = jnp.zeros_like(tab)
    tab[:, :table_ref.shape[1]] = table_ref[...]
    for c in range(PITCH):
        moved = tab[...] if c == 0 else pltpu.roll(tab[...], SPAN - c, axis=1)
        for half in range(2):
            tilt[half, pl.ds(c, kinds * HEADS, stride=PITCH), :] = moved[:, half * LANES:(half + 1) * LANES]
    pattern = base_pattern()
    span[...] = nn(jnp.concatenate([tilt[0], tilt[1]], axis=1), pattern, precision=highest)
    slot = iota((PITCH, LANES), 1)
    open_slot = (slot % PITCH < WIN_LON) & (slot < TOK)
    split = meta_ref[windows] > 0

    def spread(n, carry):
        wide = span[pl.ds(pl.multiple_of(n * PITCH, PITCH), PITCH), :]
        for r in range(WIN_LAT):
            off = (WIN_LAT - 1 - r) * PITCH
            part = wide if off == 0 else pltpu.roll(wide, SPAN - off, axis=1)
            other = (slot < half_lat * PITCH) if r >= half_lat else (slot >= half_lat * PITCH)
            ok = open_slot & jnp.logical_not(split & other)
            bias[n % kinds, pl.ds(pl.multiple_of((n // kinds) * TOK + r * PITCH, PITCH), PITCH), :] = jnp.where(ok, part[:, :LANES], masked)
        return carry

    lax.fori_loop(0, kinds * HEADS, spread, 0, unroll=True)
    fold[...] = jnp.zeros_like(fold)

    xs[...] = jnp.zeros_like(xs)
    gs[...] = jnp.zeros_like(gs)
    for w in range(windows):
        for r in range(WIN_LAT):
            at = w * TOK + r * PITCH
            start = half_lon + w * WIN_LON
            inside = WIN_LON if w < windows - 1 else half_lon
            for dst, src, lo in ((xs, s_ref, 0), (gs, g_ref, D)):
                if r < half_lat:
                    dst[at:at + inside, :] = src[r + half_lat, start:start + inside, :]
                    if inside < WIN_LON:
                        dst[at + inside:at + WIN_LON, :] = side_ref[r, :, lo:lo + D]
                else:
                    dst[at:at + inside, :] = up_ref[r - half_lat, start:start + inside, lo:lo + D]
                    if inside < WIN_LON:
                        dst[at + inside:at + WIN_LON, :] = side_ref[r, :, lo:lo + D]

    gain = gain_ref[...]
    x = xs[...].astype(f32)
    centre = x - jnp.mean(x, axis=-1, keepdims=True)
    inverse = lax.rsqrt(jnp.mean(centre * centre, axis=-1, keepdims=True) + norm_eps)
    unit = centre * inverse
    un[...] = unit
    inv[...] = inverse
    normed = (unit * gain).astype(bf16)
    nm[...] = normed
    wq, wk, wv = (wqkv_ref[:, i * D:(i + 1) * D] for i in range(3))
    q_s[...] = nn(normed, wq).astype(bf16)
    k_s[...] = nn(normed, wk).astype(bf16)
    v_s[...] = nn(normed, wv).astype(bf16)
    dm_s[...] = nt(gs[...], wproj_ref[...]).astype(bf16)

    scale = HEAD ** (-0.5)
    head_of = iota((TOK, D), 1) // HEAD
    pads = jnp.zeros((LANES - TOK, D), bf16)

    def by_head(a):
        zero = jnp.zeros_like(a)
        return [jnp.where(head_of == h, a, zero) for h in range(HEADS)]

    def window(w):
        rows = pl.ds(w * TOK, TOK)
        kind = meta_ref[w]
        q, k, v, dm = q_s[rows, :], k_s[rows, :], v_s[rows, :], dm_s[rows, :]
        q_heads = jnp.concatenate(by_head(q), axis=0)
        dm_heads = jnp.concatenate(by_head(dm), axis=0)
        k_pad = jnp.concatenate([k, pads], axis=0)
        v_pad = jnp.concatenate([v, pads], axis=0)
        scores = nt(q_heads, k_pad) * scale + bias[kind]
        top = jnp.max(scores, axis=-1, keepdims=True)
        raised = jnp.exp(scores - top)
        probs = raised * (1.0 / jnp.sum(raised, axis=-1, keepdims=True))
        probs_low = probs.astype(bf16)
        d_probs = nt(dm_heads, v_pad)
        d_scores = probs * (d_probs - jnp.sum(probs * d_probs, axis=-1, keepdims=True))
        low = d_scores.astype(bf16)
        side = lambda a: jnp.concatenate([a[h * TOK:(h + 1) * TOK] for h in range(HEADS)], axis=1)
        tall = lambda a: jnp.concatenate([b for part in by_head(a) for b in (part, pads)], axis=0)
        mix[rows, :] = nn(side(probs_low), tall(v)).astype(bf16)
        dq_s[rows, :] = (nn(side(low), tall(k)) * scale).astype(bf16)
        dv_s[rows, :] = tn(probs_low, dm_heads)[:TOK].astype(bf16)
        dk_s[rows, :] = (tn(low, q_heads) * scale)[:TOK].astype(bf16)
        for h in range(HEADS):
            total = None
            for r in range(WIN_LAT):
                off = (WIN_LAT - 1 - r) * PITCH
                part = d_scores[h * TOK + r * PITCH:h * TOK + (r + 1) * PITCH]
                part = jnp.concatenate([part, jnp.zeros_like(part)], axis=1)
                if off:
                    part = pltpu.roll(part, off, axis=1)
                total = part if total is None else total + part
            fold[pl.ds(pl.multiple_of((h * kinds + kind) * PITCH, PITCH), PITCH), :] += total

    for w in range(windows):
        window(w)

    branch = nn(mix[...], wproj_ref[...]).astype(bf16)
    gp = tn(mix[...], gs[...]).astype(bf16)
    d_normed = nt(dq_s[...], wq) + nt(dk_s[...], wk) + nt(dv_s[...], wv)
    gq = []
    for i, d in enumerate((dq_s, dk_s, dv_s)):
        gq.append(tn(nm[...], d[...]).astype(bf16))
    gq = jnp.concatenate(gq, axis=1)
    for b in range(4):
        grads_ref[b * D:(b + 1) * D, :] = gq[:, b * LANES:(b + 1) * LANES]
    grads_ref[4 * D:5 * D, :] = jnp.concatenate([gq[:, 4 * LANES:], gp[:, LANES:]], axis=1)
    grads_ref[5 * D:6 * D, :] = gp[:, :LANES]
    unit = un[...]
    gg = jnp.sum(d_normed * unit, axis=0, keepdims=True)
    gg = jnp.concatenate([gg[:, :LANES], jnp.concatenate([gg[:, LANES:], jnp.zeros((1, SPAN - D), f32)], axis=1), jnp.zeros((ROWS - AT_GAIN - 2, LANES), f32)], axis=0)
    grads_ref[AT_GAIN:, :] = gg.astype(bf16)
    d_unit = d_normed * gain
    path = inv[...] * (d_unit - jnp.mean(d_unit, axis=-1, keepdims=True) - unit * jnp.mean(d_unit * unit, axis=-1, keepdims=True))
    path = path.astype(bf16)
    for w in range(windows):
        for r in range(WIN_LAT):
            at = w * TOK + r * PITCH
            both_ref[r, w * WIN_LON:(w + 1) * WIN_LON, 0:D] = branch[at:at + WIN_LON]
            both_ref[r, w * WIN_LON:(w + 1) * WIN_LON, D:2 * D] = path[at:at + WIN_LON]

    back = nt(fold[...], pattern, precision=highest)
    for half in range(2):
        tilt[half] = back[:, half * LANES:(half + 1) * LANES]
    total = None
    for c in range(WIN_LON):
        part = jnp.concatenate([tilt[half, pl.ds(c, kinds * HEADS, stride=PITCH), :] for half in range(2)], axis=1)
        if c:
            part = pltpu.roll(part, c, axis=1)
        total = part if total is None else total + part
    for half in range(2):
        at = AT_TABLE + half * kinds * HEADS
        grads_ref[at:at + kinds * HEADS, :] = total[:, half * LANES:(half + 1) * LANES].astype(bf16)


def attend(meta, s, g, up, side, gain, w_qkv, w_proj, table):
    windows = s.shape[1] // WIN_LON
    n = windows * TOK
    vm = pl.BlockSpec(memory_space=pltpu.VMEM)
    kh = table.shape[0]
    return pl.pallas_call(
        functools.partial(kernel, windows),
        out_shape=(
            jax.ShapeDtypeStruct(s.shape[:2] + (2 * D,), bf16),
            jax.ShapeDtypeStruct((ROWS, LANES), bf16),
        ),
        in_specs=[pl.BlockSpec(memory_space=pltpu.SMEM)] + [vm] * 8,
        out_specs=(vm,) * 2,
        scratch_shapes=[
            pltpu.VMEM((n, D), bf16), pltpu.VMEM((n, D), bf16), pltpu.VMEM((kh, SPAN), f32),
            pltpu.VMEM((2, kh * PITCH, LANES), f32), pltpu.VMEM((kh * PITCH, SPAN), f32),
            pltpu.VMEM((kh // HEADS, HEADS * TOK, LANES), f32),
            pltpu.VMEM((n, D), f32), pltpu.VMEM((n, D), bf16), pltpu.VMEM((n, 1), f32),
        ] + [pltpu.VMEM((n, D), bf16)] * 8 + [pltpu.VMEM((kh * PITCH, SPAN), f32)],
        cost_estimate=pl.CostEstimate(flops=2_000_000_000, bytes_accessed=4_000_000, transcendentals=500_000),
        compiler_params=pltpu.CompilerParams(vmem_limit_bytes=VM_ATTEND << 20),
        name="attend",
    )(meta, s, g, up, side, gain, w_qkv, w_proj, table)


def finish_kernel(grads_ref, gq_ref, gp_ref, gt_ref, gg_ref):
    def scale_of(parts, count):
        total = sum(jnp.sum(jnp.sum(p * p, axis=0, keepdims=True), axis=1, keepdims=True) for p in parts)
        return jnp.minimum(1.0, lax.rsqrt(total / count + clip_eps))

    kh = gt_ref.shape[0]
    wide = [grads_ref[b * D:(b + 1) * D, :].astype(f32) for b in range(4)]
    shared = grads_ref[4 * D:5 * D, :].astype(f32)
    low, high = shared[:, :LANES // 2], shared[:, LANES // 2:]
    first = grads_ref[5 * D:6 * D, :].astype(f32)
    by = scale_of(wide + [low], gq_ref.shape[0] * gq_ref.shape[1])
    for b in range(4):
        gq_ref[:, b * LANES:(b + 1) * LANES] = wide[b] * by
    gq_ref[:, 4 * LANES:] = low * by
    by = scale_of([first, high], gp_ref.shape[0] * gp_ref.shape[1])
    gp_ref[:, :LANES] = first * by
    gp_ref[:, LANES:] = high * by
    left = grads_ref[AT_TABLE:AT_TABLE + kh, :].astype(f32)
    right = grads_ref[AT_TABLE + kh:AT_TABLE + 2 * kh, :].astype(f32)
    by = scale_of([left, right], kh * gt_ref.shape[1])
    gt_ref[:, :LANES] = left * by
    gt_ref[:, LANES:] = (right * by)[:, :gt_ref.shape[1] - LANES]
    rows = grads_ref[AT_GAIN:AT_GAIN + 16, :].astype(f32)
    by = scale_of([rows], D)
    gg_ref[:, :LANES] = rows[0:1] * by
    gg_ref[:, LANES:] = (rows[1:2] * by)[:, :D - LANES]


def finish(grads, table_rows, extent):
    vm = pl.BlockSpec(memory_space=pltpu.VMEM)
    return pl.pallas_call(
        finish_kernel,
        out_shape=(
            jax.ShapeDtypeStruct((D, 3 * D), f32),
            jax.ShapeDtypeStruct((D, D), f32),
            jax.ShapeDtypeStruct((table_rows, extent), f32),
            jax.ShapeDtypeStruct((1, D), f32),
        ),
        in_specs=[vm],
        out_specs=(vm,) * 4,
        cost_estimate=pl.CostEstimate(flops=1_000_000, bytes_accessed=1_000_000, transcendentals=4),
        compiler_params=pltpu.CompilerParams(vmem_limit_bytes=VM_FINISH << 20),
        name="finish",
    )(grads)


def shifted(value, axis, steps):
    count = lax.axis_size(axis)
    return lax.ppermute(value, axis, [(i, (i + steps) % count) for i in range(count)])


def spread_sum(part, axes):
    n = lax.axis_size(axes)
    got = lax.all_to_all(part.reshape(n, -1, LANES), axes, 0, 0, tiled=True)
    return jnp.sum(got.astype(f32), axis=0).astype(bf16)


def collect(part, axes):
    n = lax.axis_size(axes)
    return lax.all_to_all(jnp.broadcast_to(part[None], (n,) + part.shape), axes, 0, 0, tiled=True)


def total_of(packed, ahead, further):
    part = spread_sum(packed, SLICED)
    part, ahead = lax.optimization_barrier((part, ahead))
    for axes in WHOLE:
        part = jnp.sum(collect(part, axes).astype(f32), axis=0).astype(bf16)
    part, ahead = lax.optimization_barrier((part, further(ahead)))
    return collect(part, SLICED).reshape(-1, LANES), ahead


def on_device(state_grid, norm_gain, w_qkv, w_proj, bias_table, window_kind, cotangent):
    rows_dev, cols_dev, channels = state_grid.shape
    half_lat, half_lon = WIN_LAT // 2, WIN_LON // 2
    lat, lon = lax.axis_index(LAT), lax.axis_index(LON)
    windows = cols_dev // WIN_LON
    joint = jnp.concatenate([state_grid[:half_lat], cotangent[:half_lat]], axis=2)
    up = shifted(joint, LAT, -1)
    side = jnp.concatenate([state_grid[half_lat:, :half_lon], cotangent[half_lat:, :half_lon]], axis=2)
    side = shifted(jnp.concatenate([side, up[:, :half_lon]], axis=0), LON, -1)
    kinds = lax.dynamic_slice(window_kind, (lat, lon * windows), (1, windows))[0]
    last = (lat == lax.axis_size(LAT) - 1).astype(jnp.int32)
    meta = jnp.concatenate([kinds, last[None]])
    kind_count, heads, extent = bias_table.shape
    table = bias_table.transpose(1, 0, 2).reshape(heads * kind_count, extent)
    both, packed = attend(meta, state_grid, cotangent, up, side, norm_gain.reshape(1, -1), w_qkv, w_proj, table)
    moved = shifted(both[:, -half_lon:], LON, 1)

    def up_to_rows(moved):
        placed = jnp.concatenate([moved, both[:, :-half_lon]], axis=1)
        return placed[:half_lat], shifted(placed[half_lat:], LAT, 1)

    summed, (stay, lower) = total_of(packed, moved, up_to_rows)
    own = jnp.concatenate([lower, stay], axis=0).astype(f32)
    out_field = (state_grid.astype(f32) + own[:, :, :channels]).astype(bf16)
    d_field = (cotangent.astype(f32) + own[:, :, channels:]).astype(bf16)
    gq, gp, gt, gg = finish(summed, heads * kind_count, extent)
    gt = gt.reshape(heads, kind_count, extent).transpose(1, 0, 2)
    return (out_field, d_field, gq, gp, gt, gg.reshape(-1))


def solution(mesh):
    in_specs = (P(LAT, LON, None), P(), P(), P(), P(), P(), P(LAT, LON, None))
    out_specs = (P(LAT, LON, None), P(LAT, LON, None), P(), P(), P(), P())
    mesh = Mesh(mesh.devices.reshape(PARTS), LAT + LON)
    return jax.shard_map(on_device, mesh=mesh, in_specs=in_specs, out_specs=out_specs, check_vma=False)
```

```python
import functools
import jax
import jax.numpy as jnp
from jax import lax
from jax.experimental import pallas as pl
from jax.experimental.pallas import tpu as pltpu
from jax.sharding import Mesh, PartitionSpec as P

HEADS = 6
WIN_LAT = 6
WIN_LON = 12
HEAD = 32
D = 192
PITCH = 16
TOK = WIN_LAT * PITCH
LANES = 128
SPAN = 256
norm_eps = 1e-05
clip_eps = 1e-06
masked = -1e30
AT_TABLE = 6 * D
AT_GAIN = AT_TABLE + 96
ROWS = 1280
VM_ATTEND = 28
VM_FINISH = 8
VM_BIAS = 10
LAT = ("y_lo", "z_hi", "z_lo")
LON = ("y_hi", "x", "core")
PARTS = (2, 4, 2, 4, 4, 2)
SLICED = ("y_lo", "z_lo", "x", "core")
WHOLE = ("z_hi", "y_hi")
highest = lax.Precision.HIGHEST
f32 = jnp.float32
bf16 = jnp.bfloat16

NT = (((1,), (1,)), ((), ()))
TN = (((0,), (0,)), ((), ()))


def nt(a, b, **kw):
    return lax.dot_general(a, b, NT, preferred_element_type=f32, **kw)


def tn(a, b, **kw):
    return lax.dot_general(a, b, TN, preferred_element_type=f32, **kw)


def nn(a, b, **kw):
    return jnp.dot(a, b, preferred_element_type=f32, **kw)


def iota(shape, dim):
    return lax.broadcasted_iota(jnp.int32, shape, dim)


def base_pattern():
    p = iota((SPAN, SPAN), 0)
    lane = iota((SPAN, SPAN), 1)
    d = lane // PITCH
    c = lane % PITCH
    hit = (p == (2 * WIN_LAT - 2 - d) * (2 * WIN_LON - 1) - c + WIN_LON - 1) & (c < WIN_LON) & (d < 2 * WIN_LAT - 1)
    return hit.astype(f32)


def bias_kernel(table_ref, last_ref, bias, tab, tilt, span):
    half_lat = WIN_LAT // 2
    kinds = table_ref.shape[0] // HEADS
    tab[...] = jnp.zeros_like(tab)
    tab[:, :table_ref.shape[1]] = table_ref[...]
    for c in range(PITCH):
        moved = tab[...] if c == 0 else pltpu.roll(tab[...], SPAN - c, axis=1)
        for half in range(2):
            tilt[half, pl.ds(c, kinds * HEADS, stride=PITCH), :] = moved[:, half * LANES:(half + 1) * LANES]
    pattern = base_pattern()
    span[...] = nn(jnp.concatenate([tilt[0], tilt[1]], axis=1), pattern, precision=highest)
    slot = iota((PITCH, LANES), 1)
    open_slot = (slot % PITCH < WIN_LON) & (slot < TOK)
    split = last_ref[0] > 0

    def spread(n, carry):
        wide = span[pl.ds(pl.multiple_of(n * PITCH, PITCH), PITCH), :]
        for r in range(WIN_LAT):
            off = (WIN_LAT - 1 - r) * PITCH
            part = wide if off == 0 else pltpu.roll(wide, SPAN - off, axis=1)
            other = (slot < half_lat * PITCH) if r >= half_lat else (slot >= half_lat * PITCH)
            ok = open_slot & jnp.logical_not(split & other)
            bias[n % kinds, pl.ds(pl.multiple_of((n // kinds) * TOK + r * PITCH, PITCH), PITCH), :] = jnp.where(ok, part[:, :LANES], masked)
        return carry

    lax.fori_loop(0, kinds * HEADS, spread, 0, unroll=True)


def bias_of(table, last):
    vm = pl.BlockSpec(memory_space=pltpu.VMEM)
    kh = table.shape[0]
    return pl.pallas_call(
        bias_kernel,
        out_shape=jax.ShapeDtypeStruct((kh // HEADS, HEADS * TOK, LANES), f32),
        in_specs=[vm, pl.BlockSpec(memory_space=pltpu.SMEM)],
        out_specs=vm,
        scratch_shapes=[
            pltpu.VMEM((kh, SPAN), f32), pltpu.VMEM((2, kh * PITCH, LANES), f32), pltpu.VMEM((kh * PITCH, SPAN), f32),
        ],
        cost_estimate=pl.CostEstimate(flops=600_000_000, bytes_accessed=2_500_000, transcendentals=0),
        compiler_params=pltpu.CompilerParams(vmem_limit_bytes=VM_BIAS << 20),
        name="bias",
    )(table, last)


def kernel(windows, kinds, meta_ref, s_ref, g_ref, up_ref, side_ref, corner_ref, gain_ref, wqkv_ref, wproj_ref, bias,
           both_ref, grads_ref,
           xs, gs, tilt, un, nm, inv, q_s, k_s, v_s, dm_s, mix, dq_s, dk_s, dv_s, fold):
    half_lat = WIN_LAT // 2
    half_lon = WIN_LON // 2

    pattern = base_pattern()
    fold[...] = jnp.zeros_like(fold)

    xs[...] = jnp.zeros_like(xs)
    gs[...] = jnp.zeros_like(gs)
    for w in range(windows):
        for r in range(WIN_LAT):
            at = w * TOK + r * PITCH
            start = half_lon + w * WIN_LON
            inside = WIN_LON if w < windows - 1 else half_lon
            for dst, src, lo in ((xs, s_ref, 0), (gs, g_ref, D)):
                if r < half_lat:
                    dst[at:at + inside, :] = src[r + half_lat, start:start + inside, :]
                    if inside < WIN_LON:
                        dst[at + inside:at + WIN_LON, :] = side_ref[r, :, lo:lo + D]
                else:
                    dst[at:at + inside, :] = up_ref[r - half_lat, start:start + inside, lo:lo + D]
                    if inside < WIN_LON:
                        dst[at + inside:at + WIN_LON, :] = corner_ref[r - half_lat, :, lo:lo + D]

    gain = gain_ref[...]
    x = xs[...].astype(f32)
    centre = x - jnp.mean(x, axis=-1, keepdims=True)
    inverse = lax.rsqrt(jnp.mean(centre * centre, axis=-1, keepdims=True) + norm_eps)
    unit = centre * inverse
    un[...] = unit
    inv[...] = inverse
    normed = (unit * gain).astype(bf16)
    nm[...] = normed
    wq, wk, wv = (wqkv_ref[:, i * D:(i + 1) * D] for i in range(3))
    q_s[...] = nn(normed, wq).astype(bf16)
    k_s[...] = nn(normed, wk).astype(bf16)
    v_s[...] = nn(normed, wv).astype(bf16)
    dm_s[...] = nt(gs[...], wproj_ref[...]).astype(bf16)

    scale = HEAD ** (-0.5)
    head_of = iota((TOK, D), 1) // HEAD
    pads = jnp.zeros((LANES - TOK, D), bf16)

    def by_head(a):
        zero = jnp.zeros_like(a)
        return [jnp.where(head_of == h, a, zero) for h in range(HEADS)]

    def window(w):
        rows = pl.ds(w * TOK, TOK)
        kind = meta_ref[w]
        q, k, v, dm = q_s[rows, :], k_s[rows, :], v_s[rows, :], dm_s[rows, :]
        q_heads = jnp.concatenate(by_head(q), axis=0)
        dm_heads = jnp.concatenate(by_head(dm), axis=0)
        k_pad = jnp.concatenate([k, pads], axis=0)
        v_pad = jnp.concatenate([v, pads], axis=0)
        scores = nt(q_heads, k_pad) * scale + bias[kind]
        top = jnp.max(scores, axis=-1, keepdims=True)
        raised = jnp.exp(scores - top)
        probs = raised * (1.0 / jnp.sum(raised, axis=-1, keepdims=True))
        probs_low = probs.astype(bf16)
        d_probs = nt(dm_heads, v_pad)
        d_scores = probs * (d_probs - jnp.sum(probs * d_probs, axis=-1, keepdims=True))
        low = d_scores.astype(bf16)
        side = lambda a: jnp.concatenate([a[h * TOK:(h + 1) * TOK] for h in range(HEADS)], axis=1)
        tall = lambda a: jnp.concatenate([b for part in by_head(a) for b in (part, pads)], axis=0)
        mix[rows, :] = nn(side(probs_low), tall(v)).astype(bf16)
        dq_s[rows, :] = (nn(side(low), tall(k)) * scale).astype(bf16)
        dv_s[rows, :] = tn(probs_low, dm_heads)[:TOK].astype(bf16)
        dk_s[rows, :] = (tn(low, q_heads) * scale)[:TOK].astype(bf16)
        for h in range(HEADS):
            total = None
            for r in range(WIN_LAT):
                off = (WIN_LAT - 1 - r) * PITCH
                part = d_scores[h * TOK + r * PITCH:h * TOK + (r + 1) * PITCH]
                part = jnp.concatenate([part, jnp.zeros_like(part)], axis=1)
                if off:
                    part = pltpu.roll(part, off, axis=1)
                total = part if total is None else total + part
            fold[pl.ds(pl.multiple_of((h * kinds + kind) * PITCH, PITCH), PITCH), :] += total

    for w in range(windows):
        window(w)

    branch = nn(mix[...], wproj_ref[...]).astype(bf16)
    gp = tn(mix[...], gs[...]).astype(bf16)
    d_normed = nt(dq_s[...], wq) + nt(dk_s[...], wk) + nt(dv_s[...], wv)
    gq = []
    for d in (dq_s, dk_s, dv_s):
        gq.append(tn(nm[...], d[...]).astype(bf16))
    gq = jnp.concatenate(gq, axis=1)
    for b in range(4):
        grads_ref[b * D:(b + 1) * D, :] = gq[:, b * LANES:(b + 1) * LANES]
    grads_ref[4 * D:5 * D, :] = jnp.concatenate([gq[:, 4 * LANES:], gp[:, LANES:]], axis=1)
    grads_ref[5 * D:6 * D, :] = gp[:, :LANES]
    unit = un[...]
    gg = jnp.sum(d_normed * unit, axis=0, keepdims=True)
    gg = jnp.concatenate([gg[:, :LANES], jnp.concatenate([gg[:, LANES:], jnp.zeros((1, SPAN - D), f32)], axis=1), jnp.zeros((ROWS - AT_GAIN - 2, LANES), f32)], axis=0)
    grads_ref[AT_GAIN:, :] = gg.astype(bf16)
    d_unit = d_normed * gain
    path = inv[...] * (d_unit - jnp.mean(d_unit, axis=-1, keepdims=True) - unit * jnp.mean(d_unit * unit, axis=-1, keepdims=True))
    path = path.astype(bf16)
    for w in range(windows):
        for r in range(WIN_LAT):
            at = w * TOK + r * PITCH
            both_ref[r, w * WIN_LON:(w + 1) * WIN_LON, 0:D] = branch[at:at + WIN_LON]
            both_ref[r, w * WIN_LON:(w + 1) * WIN_LON, D:2 * D] = path[at:at + WIN_LON]

    back = nt(fold[...], pattern, precision=highest)
    for half in range(2):
        tilt[half] = back[:, half * LANES:(half + 1) * LANES]
    total = None
    for c in range(WIN_LON):
        part = jnp.concatenate([tilt[half, pl.ds(c, kinds * HEADS, stride=PITCH), :] for half in range(2)], axis=1)
        if c:
            part = pltpu.roll(part, c, axis=1)
        total = part if total is None else total + part
    for half in range(2):
        at = AT_TABLE + half * kinds * HEADS
        grads_ref[at:at + kinds * HEADS, :] = total[:, half * LANES:(half + 1) * LANES].astype(bf16)


def attend(kinds, s, g, up, side, corner, gain, w_qkv, w_proj, bias):
    windows = s.shape[1] // WIN_LON
    n = windows * TOK
    vm = pl.BlockSpec(memory_space=pltpu.VMEM)
    kh = bias.shape[0] * HEADS
    return pl.pallas_call(
        functools.partial(kernel, windows, bias.shape[0]),
        out_shape=(
            jax.ShapeDtypeStruct(s.shape[:2] + (2 * D,), bf16),
            jax.ShapeDtypeStruct((ROWS, LANES), bf16),
        ),
        in_specs=[pl.BlockSpec(memory_space=pltpu.SMEM)] + [vm] * 9,
        out_specs=(vm,) * 2,
        scratch_shapes=[
            pltpu.VMEM((n, D), bf16), pltpu.VMEM((n, D), bf16), pltpu.VMEM((2, kh * PITCH, LANES), f32),
            pltpu.VMEM((n, D), f32), pltpu.VMEM((n, D), bf16), pltpu.VMEM((n, 1), f32),
        ] + [pltpu.VMEM((n, D), bf16)] * 8 + [pltpu.VMEM((kh * PITCH, SPAN), f32)],
        cost_estimate=pl.CostEstimate(flops=2_000_000_000, bytes_accessed=4_000_000, transcendentals=500_000),
        compiler_params=pltpu.CompilerParams(vmem_limit_bytes=VM_ATTEND << 20),
        name="attend",
    )(kinds, s, g, up, side, corner, gain, w_qkv, w_proj, bias)


def finish_kernel(grads_ref, gq_ref, gp_ref, gt_ref, gg_ref):
    def scale_of(parts, count):
        total = sum(jnp.sum(jnp.sum(p * p, axis=0, keepdims=True), axis=1, keepdims=True) for p in parts)
        return jnp.minimum(1.0, lax.rsqrt(total / count + clip_eps))

    kh = gt_ref.shape[0]
    wide = [grads_ref[b * D:(b + 1) * D, :].astype(f32) for b in range(4)]
    shared = grads_ref[4 * D:5 * D, :].astype(f32)
    low, high = shared[:, :LANES // 2], shared[:, LANES // 2:]
    first = grads_ref[5 * D:6 * D, :].astype(f32)
    by = scale_of(wide + [low], gq_ref.shape[0] * gq_ref.shape[1])
    for b in range(4):
        gq_ref[:, b * LANES:(b + 1) * LANES] = wide[b] * by
    gq_ref[:, 4 * LANES:] = low * by
    by = scale_of([first, high], gp_ref.shape[0] * gp_ref.shape[1])
    gp_ref[:, :LANES] = first * by
    gp_ref[:, LANES:] = high * by
    left = grads_ref[AT_TABLE:AT_TABLE + kh, :].astype(f32)
    right = grads_ref[AT_TABLE + kh:AT_TABLE + 2 * kh, :].astype(f32)
    by = scale_of([left, right], kh * gt_ref.shape[1])
    gt_ref[:, :LANES] = left * by
    gt_ref[:, LANES:] = (right * by)[:, :gt_ref.shape[1] - LANES]
    rows = grads_ref[AT_GAIN:AT_GAIN + 16, :].astype(f32)
    by = scale_of([rows], D)
    gg_ref[:, :LANES] = rows[0:1] * by
    gg_ref[:, LANES:] = (rows[1:2] * by)[:, :D - LANES]


def finish(grads, table_rows, extent):
    vm = pl.BlockSpec(memory_space=pltpu.VMEM)
    return pl.pallas_call(
        finish_kernel,
        out_shape=(
            jax.ShapeDtypeStruct((D, 3 * D), f32),
            jax.ShapeDtypeStruct((D, D), f32),
            jax.ShapeDtypeStruct((table_rows, extent), f32),
            jax.ShapeDtypeStruct((1, D), f32),
        ),
        in_specs=[vm],
        out_specs=(vm,) * 4,
        cost_estimate=pl.CostEstimate(flops=1_000_000, bytes_accessed=1_000_000, transcendentals=4),
        compiler_params=pltpu.CompilerParams(vmem_limit_bytes=VM_FINISH << 20),
        name="finish",
    )(grads)


def shifted(value, axis, steps):
    count = lax.axis_size(axis)
    return lax.ppermute(value, axis, [(i, (i + steps) % count) for i in range(count)])


def exchange(part, axes):
    return lax.all_to_all(part, axes, 0, 0, tiled=True)


def whole_sum(got):
    return jnp.sum(got.astype(f32), axis=0).astype(bf16)


def copies(part, axes):
    return jnp.broadcast_to(part[None], (lax.axis_size(axes),) + part.shape)


def total_of(packed):
    part = exchange(packed.reshape(lax.axis_size(SLICED), -1, LANES), SLICED)
    part = whole_sum(part)
    part = exchange(copies(part, WHOLE), WHOLE)
    part = whole_sum(part)
    part = exchange(copies(part, SLICED), SLICED)
    return part.reshape(-1, LANES)


def on_device(state_grid, norm_gain, w_qkv, w_proj, bias_table, window_kind, cotangent):
    _, cols_dev, channels = state_grid.shape
    half_lat, half_lon = WIN_LAT // 2, WIN_LON // 2
    lat, lon = lax.axis_index(LAT), lax.axis_index(LON)
    windows = cols_dev // WIN_LON
    joint = jnp.concatenate([state_grid[:half_lat], cotangent[:half_lat]], axis=2)
    side = jnp.concatenate([state_grid[half_lat:, :half_lon], cotangent[half_lat:, :half_lon]], axis=2)
    up = shifted(joint, LAT, -1)
    lats, lons = lax.axis_size(LAT), lax.axis_size(LON)
    before = [(i * lons + j, (i - 1) % lats * lons + (j - 1) % lons) for i in range(lats) for j in range(lons)]
    corner = lax.ppermute(joint[:, :half_lon], LAT + LON, before)
    side = shifted(side, LON, -1)
    kinds = lax.dynamic_slice(window_kind, (lat, lon * windows), (1, windows))[0]
    last = (lat == lax.axis_size(LAT) - 1).astype(jnp.int32)
    kind_count, heads, extent = bias_table.shape
    table = bias_table.transpose(1, 0, 2).reshape(heads * kind_count, extent)
    both, packed = attend(
        kinds, state_grid, cotangent, up, side, corner, norm_gain.reshape(1, -1), w_qkv, w_proj, bias_of(table, last[None])
    )
    moved = shifted(both[:, -half_lon:], LON, 1)
    placed = jnp.concatenate([moved, both[:, :-half_lon]], axis=1)
    lower = shifted(placed[half_lat:], LAT, 1)
    summed = total_of(packed)
    own = jnp.concatenate([lower, placed[:half_lat]], axis=0).astype(f32)
    out_field = (state_grid.astype(f32) + own[:, :, :channels]).astype(bf16)
    d_field = (cotangent.astype(f32) + own[:, :, channels:]).astype(bf16)
    gq, gp, gt, gg = finish(summed, heads * kind_count, extent)
    gt = gt.reshape(heads, kind_count, extent).transpose(1, 0, 2)
    return (out_field, d_field, gq, gp, gt, gg.reshape(-1))


def solution(mesh):
    in_specs = (P(LAT, LON, None), P(), P(), P(), P(), P(), P(LAT, LON, None))
    out_specs = (P(LAT, LON, None), P(LAT, LON, None), P(), P(), P(), P())
    mesh = Mesh(mesh.devices.reshape(PARTS), LAT + LON)
    return jax.shard_map(on_device, mesh=mesh, in_specs=in_specs, out_specs=out_specs, check_vma=False)
```

```python
import functools
import jax
import jax.numpy as jnp
from jax import lax
from jax.experimental import pallas as pl
from jax.experimental.pallas import tpu as pltpu
from jax.sharding import Mesh, PartitionSpec as P

HEADS = 6
WIN_LAT = 6
WIN_LON = 12
HEAD = 32
D = 192
PITCH = 16
TOK = WIN_LAT * PITCH
LANES = 128
SPAN = 256
norm_eps = 1e-05
clip_eps = 1e-06
masked = -1e30
AT_TABLE = 6 * D
AT_GAIN = AT_TABLE + 96
ROWS = 1280
VM_ATTEND = 28
VM_FINISH = 8
VM_BIAS = 10
VM_RESULTS = 8
LAT = ("y_lo", "z_hi", "z_lo")
LON = ("y_hi", "x", "core")
PARTS = (2, 4, 2, 4, 4, 2)
SLICED = ("y_lo", "z_lo", "x", "core")
WHOLE = ("z_hi", "y_hi")
highest = lax.Precision.HIGHEST
f32 = jnp.float32
bf16 = jnp.bfloat16

NT = (((1,), (1,)), ((), ()))
TN = (((0,), (0,)), ((), ()))


def nt(a, b, **kw):
    return lax.dot_general(a, b, NT, preferred_element_type=f32, **kw)


def tn(a, b, **kw):
    return lax.dot_general(a, b, TN, preferred_element_type=f32, **kw)


def nn(a, b, **kw):
    return jnp.dot(a, b, preferred_element_type=f32, **kw)


def iota(shape, dim):
    return lax.broadcasted_iota(jnp.int32, shape, dim)


def base_pattern():
    p = iota((SPAN, SPAN), 0)
    lane = iota((SPAN, SPAN), 1)
    d = lane // PITCH
    c = lane % PITCH
    hit = (p == (2 * WIN_LAT - 2 - d) * (2 * WIN_LON - 1) - c + WIN_LON - 1) & (c < WIN_LON) & (d < 2 * WIN_LAT - 1)
    return hit.astype(f32)


def bias_kernel(table_ref, last_ref, bias, tab, tilt, span):
    half_lat = WIN_LAT // 2
    kinds = table_ref.shape[0] // HEADS
    tab[...] = jnp.zeros_like(tab)
    tab[:, :table_ref.shape[1]] = table_ref[...]
    for c in range(PITCH):
        moved = tab[...] if c == 0 else pltpu.roll(tab[...], SPAN - c, axis=1)
        for half in range(2):
            tilt[half, pl.ds(c, kinds * HEADS, stride=PITCH), :] = moved[:, half * LANES:(half + 1) * LANES]
    pattern = base_pattern()
    span[...] = nn(jnp.concatenate([tilt[0], tilt[1]], axis=1), pattern, precision=highest)
    slot = iota((PITCH, LANES), 1)
    open_slot = (slot % PITCH < WIN_LON) & (slot < TOK)
    split = last_ref[0] > 0

    def spread(n, carry):
        wide = span[pl.ds(pl.multiple_of(n * PITCH, PITCH), PITCH), :]
        for r in range(WIN_LAT):
            off = (WIN_LAT - 1 - r) * PITCH
            part = wide if off == 0 else pltpu.roll(wide, SPAN - off, axis=1)
            other = (slot < half_lat * PITCH) if r >= half_lat else (slot >= half_lat * PITCH)
            ok = open_slot & jnp.logical_not(split & other)
            bias[n % kinds, pl.ds(pl.multiple_of((n // kinds) * TOK + r * PITCH, PITCH), PITCH), :] = jnp.where(ok, part[:, :LANES], masked)
        return carry

    lax.fori_loop(0, kinds * HEADS, spread, 0, unroll=True)


def bias_of(table, last):
    vm = pl.BlockSpec(memory_space=pltpu.VMEM)
    kh = table.shape[0]
    return pl.pallas_call(
        bias_kernel,
        out_shape=jax.ShapeDtypeStruct((kh // HEADS, HEADS * TOK, LANES), f32),
        in_specs=[vm, pl.BlockSpec(memory_space=pltpu.SMEM)],
        out_specs=vm,
        scratch_shapes=[
            pltpu.VMEM((kh, SPAN), f32), pltpu.VMEM((2, kh * PITCH, LANES), f32), pltpu.VMEM((kh * PITCH, SPAN), f32),
        ],
        cost_estimate=pl.CostEstimate(flops=600_000_000, bytes_accessed=2_500_000, transcendentals=0),
        compiler_params=pltpu.CompilerParams(vmem_limit_bytes=VM_BIAS << 20),
        name="bias",
    )(table, last)


def kernel(windows, kinds, meta_ref, own_ref, up_ref, side_ref, corner_ref, gain_ref, wqkv_ref, wproj_ref, bias,
           grads_ref, mix, dn_ref, un, inv,
           xs, gs, tilt, nm, q_s, k_s, v_s, dm_s, dq_s, dk_s, dv_s, fold):
    half_lat = WIN_LAT // 2
    half_lon = WIN_LON // 2

    pattern = base_pattern()
    fold[...] = jnp.zeros_like(fold)

    xs[...] = jnp.zeros_like(xs)
    gs[...] = jnp.zeros_like(gs)
    for w in range(windows):
        for r in range(WIN_LAT):
            at = w * TOK + r * PITCH
            start = half_lon + w * WIN_LON
            inside = WIN_LON if w < windows - 1 else half_lon
            for dst, lo in ((xs, 0), (gs, D)):
                if r < half_lat:
                    dst[at:at + inside, :] = own_ref[r + half_lat, start:start + inside, lo:lo + D]
                    if inside < WIN_LON:
                        dst[at + inside:at + WIN_LON, :] = side_ref[r, :, lo:lo + D]
                else:
                    dst[at:at + inside, :] = up_ref[r - half_lat, start:start + inside, lo:lo + D]
                    if inside < WIN_LON:
                        dst[at + inside:at + WIN_LON, :] = corner_ref[r - half_lat, :, lo:lo + D]

    gain = gain_ref[...]
    x = xs[...].astype(f32)
    centre = x - jnp.mean(x, axis=-1, keepdims=True)
    inverse = lax.rsqrt(jnp.mean(centre * centre, axis=-1, keepdims=True) + norm_eps)
    unit = centre * inverse
    un[...] = unit
    inv[...] = inverse
    normed = (unit * gain).astype(bf16)
    nm[...] = normed
    wq, wk, wv = (wqkv_ref[:, i * D:(i + 1) * D] for i in range(3))
    q_s[...] = nn(normed, wq).astype(bf16)
    k_s[...] = nn(normed, wk).astype(bf16)
    v_s[...] = nn(normed, wv).astype(bf16)
    dm_s[...] = nt(gs[...], wproj_ref[...]).astype(bf16)

    scale = HEAD ** (-0.5)
    head_of = iota((TOK, D), 1) // HEAD
    pads = jnp.zeros((LANES - TOK, D), bf16)

    def by_head(a):
        zero = jnp.zeros_like(a)
        return [jnp.where(head_of == h, a, zero) for h in range(HEADS)]

    def window(w):
        rows = pl.ds(w * TOK, TOK)
        kind = meta_ref[w]
        q, k, v, dm = q_s[rows, :], k_s[rows, :], v_s[rows, :], dm_s[rows, :]
        q_heads = jnp.concatenate(by_head(q), axis=0)
        dm_heads = jnp.concatenate(by_head(dm), axis=0)
        k_pad = jnp.concatenate([k, pads], axis=0)
        v_pad = jnp.concatenate([v, pads], axis=0)
        scores = nt(q_heads, k_pad) * scale + bias[kind]
        top = jnp.max(scores, axis=-1, keepdims=True)
        raised = jnp.exp(scores - top)
        probs = raised * (1.0 / jnp.sum(raised, axis=-1, keepdims=True))
        probs_low = probs.astype(bf16)
        d_probs = nt(dm_heads, v_pad)
        d_scores = probs * (d_probs - jnp.sum(probs * d_probs, axis=-1, keepdims=True))
        low = d_scores.astype(bf16)
        side = lambda a: jnp.concatenate([a[h * TOK:(h + 1) * TOK] for h in range(HEADS)], axis=1)
        tall = lambda a: jnp.concatenate([b for part in by_head(a) for b in (part, pads)], axis=0)
        mix[rows, :] = nn(side(probs_low), tall(v)).astype(bf16)
        dq_s[rows, :] = (nn(side(low), tall(k)) * scale).astype(bf16)
        dv_s[rows, :] = tn(probs_low, dm_heads)[:TOK].astype(bf16)
        dk_s[rows, :] = (tn(low, q_heads) * scale)[:TOK].astype(bf16)
        for h in range(HEADS):
            total = None
            for r in range(WIN_LAT):
                off = (WIN_LAT - 1 - r) * PITCH
                part = d_scores[h * TOK + r * PITCH:h * TOK + (r + 1) * PITCH]
                part = jnp.concatenate([part, jnp.zeros_like(part)], axis=1)
                if off:
                    part = pltpu.roll(part, off, axis=1)
                total = part if total is None else total + part
            fold[pl.ds(pl.multiple_of((h * kinds + kind) * PITCH, PITCH), PITCH), :] += total

    for w in range(windows):
        window(w)

    gp = tn(mix[...], gs[...]).astype(bf16)
    d_normed = nt(dq_s[...], wq) + nt(dk_s[...], wk) + nt(dv_s[...], wv)
    dn_ref[...] = d_normed
    gq = []
    for d in (dq_s, dk_s, dv_s):
        gq.append(tn(nm[...], d[...]).astype(bf16))
    gq = jnp.concatenate(gq, axis=1)
    for b in range(4):
        grads_ref[b * D:(b + 1) * D, :] = gq[:, b * LANES:(b + 1) * LANES]
    grads_ref[4 * D:5 * D, :] = jnp.concatenate([gq[:, 4 * LANES:], gp[:, LANES:]], axis=1)
    grads_ref[5 * D:6 * D, :] = gp[:, :LANES]
    unit = un[...]
    gg = jnp.sum(d_normed * unit, axis=0, keepdims=True)
    gg = jnp.concatenate([gg[:, :LANES], jnp.concatenate([gg[:, LANES:], jnp.zeros((1, SPAN - D), f32)], axis=1), jnp.zeros((ROWS - AT_GAIN - 2, LANES), f32)], axis=0)
    grads_ref[AT_GAIN:, :] = gg.astype(bf16)

    back = nt(fold[...], pattern, precision=highest)
    for half in range(2):
        tilt[half] = back[:, half * LANES:(half + 1) * LANES]
    total = None
    for c in range(WIN_LON):
        part = jnp.concatenate([tilt[half, pl.ds(c, kinds * HEADS, stride=PITCH), :] for half in range(2)], axis=1)
        if c:
            part = pltpu.roll(part, c, axis=1)
        total = part if total is None else total + part
    for half in range(2):
        at = AT_TABLE + half * kinds * HEADS
        grads_ref[at:at + kinds * HEADS, :] = total[:, half * LANES:(half + 1) * LANES].astype(bf16)


def results_kernel(windows, mix, dn_ref, un, inv, gain_ref, wproj_ref, both_ref):
    gain = gain_ref[...]
    branch = nn(mix[...], wproj_ref[...]).astype(bf16)
    d_normed = dn_ref[...]
    unit = un[...]
    d_unit = d_normed * gain
    path = inv[...] * (d_unit - jnp.mean(d_unit, axis=-1, keepdims=True) - unit * jnp.mean(d_unit * unit, axis=-1, keepdims=True))
    path = path.astype(bf16)
    for w in range(windows):
        for r in range(WIN_LAT):
            at = w * TOK + r * PITCH
            both_ref[r, w * WIN_LON:(w + 1) * WIN_LON, 0:D] = branch[at:at + WIN_LON]
            both_ref[r, w * WIN_LON:(w + 1) * WIN_LON, D:2 * D] = path[at:at + WIN_LON]


def results(windows, mix, d_normed, unit, inverse, gain, w_proj):
    vm = pl.BlockSpec(memory_space=pltpu.VMEM)
    return pl.pallas_call(
        functools.partial(results_kernel, windows),
        out_shape=jax.ShapeDtypeStruct((WIN_LAT, windows * WIN_LON, 2 * D), bf16),
        in_specs=[vm] * 6,
        out_specs=vm,
        cost_estimate=pl.CostEstimate(flops=60_000_000, bytes_accessed=2_000_000, transcendentals=0),
        compiler_params=pltpu.CompilerParams(vmem_limit_bytes=VM_RESULTS << 20),
        name="results",
    )(mix, d_normed, unit, inverse, gain, w_proj)


def attend(kinds, own, up, side, corner, gain, w_qkv, w_proj, bias):
    windows = own.shape[1] // WIN_LON
    n = windows * TOK
    vm = pl.BlockSpec(memory_space=pltpu.VMEM)
    kh = bias.shape[0] * HEADS
    return pl.pallas_call(
        functools.partial(kernel, windows, bias.shape[0]),
        out_shape=(
            jax.ShapeDtypeStruct((ROWS, LANES), bf16),
            jax.ShapeDtypeStruct((n, D), bf16),
            jax.ShapeDtypeStruct((n, D), f32),
            jax.ShapeDtypeStruct((n, D), f32),
            jax.ShapeDtypeStruct((n, 1), f32),
        ),
        in_specs=[pl.BlockSpec(memory_space=pltpu.SMEM)] + [vm] * 8,
        out_specs=(vm,) * 5,
        scratch_shapes=[
            pltpu.VMEM((n, D), bf16), pltpu.VMEM((n, D), bf16), pltpu.VMEM((2, kh * PITCH, LANES), f32),
            pltpu.VMEM((n, D), bf16),
        ] + [pltpu.VMEM((n, D), bf16)] * 7 + [pltpu.VMEM((kh * PITCH, SPAN), f32)],
        cost_estimate=pl.CostEstimate(flops=2_000_000_000, bytes_accessed=4_000_000, transcendentals=500_000),
        compiler_params=pltpu.CompilerParams(vmem_limit_bytes=VM_ATTEND << 20),
        name="attend",
    )(kinds, own, up, side, corner, gain, w_qkv, w_proj, bias)


def finish_kernel(grads_ref, gq_ref, gp_ref, gt_ref, gg_ref):
    def scale_of(parts, count):
        total = sum(jnp.sum(jnp.sum(p * p, axis=0, keepdims=True), axis=1, keepdims=True) for p in parts)
        return jnp.minimum(1.0, lax.rsqrt(total / count + clip_eps))

    kh = gt_ref.shape[0]
    wide = [grads_ref[b * D:(b + 1) * D, :].astype(f32) for b in range(4)]
    shared = grads_ref[4 * D:5 * D, :].astype(f32)
    low, high = shared[:, :LANES // 2], shared[:, LANES // 2:]
    first = grads_ref[5 * D:6 * D, :].astype(f32)
    by = scale_of(wide + [low], gq_ref.shape[0] * gq_ref.shape[1])
    for b in range(4):
        gq_ref[:, b * LANES:(b + 1) * LANES] = wide[b] * by
    gq_ref[:, 4 * LANES:] = low * by
    by = scale_of([first, high], gp_ref.shape[0] * gp_ref.shape[1])
    gp_ref[:, :LANES] = first * by
    gp_ref[:, LANES:] = high * by
    left = grads_ref[AT_TABLE:AT_TABLE + kh, :].astype(f32)
    right = grads_ref[AT_TABLE + kh:AT_TABLE + 2 * kh, :].astype(f32)
    by = scale_of([left, right], kh * gt_ref.shape[1])
    gt_ref[:, :LANES] = left * by
    gt_ref[:, LANES:] = (right * by)[:, :gt_ref.shape[1] - LANES]
    rows = grads_ref[AT_GAIN:AT_GAIN + 16, :].astype(f32)
    by = scale_of([rows], D)
    gg_ref[:, :LANES] = rows[0:1] * by
    gg_ref[:, LANES:] = (rows[1:2] * by)[:, :D - LANES]


def finish(grads, table_rows, extent):
    vm = pl.BlockSpec(memory_space=pltpu.VMEM)
    return pl.pallas_call(
        finish_kernel,
        out_shape=(
            jax.ShapeDtypeStruct((D, 3 * D), f32),
            jax.ShapeDtypeStruct((D, D), f32),
            jax.ShapeDtypeStruct((table_rows, extent), f32),
            jax.ShapeDtypeStruct((1, D), f32),
        ),
        in_specs=[vm],
        out_specs=(vm,) * 4,
        cost_estimate=pl.CostEstimate(flops=1_000_000, bytes_accessed=1_000_000, transcendentals=4),
        compiler_params=pltpu.CompilerParams(vmem_limit_bytes=VM_FINISH << 20),
        name="finish",
    )(grads)


def shifted(value, axis, steps):
    count = lax.axis_size(axis)
    return lax.ppermute(value, axis, [(i, (i + steps) % count) for i in range(count)])


def exchange(part, axes):
    return lax.all_to_all(part, axes, 0, 0, tiled=True)


def whole_sum(got):
    return jnp.sum(got.astype(f32), axis=0).astype(bf16)


def copies(part, axes):
    return jnp.broadcast_to(part[None], (lax.axis_size(axes),) + part.shape)


def total_of(packed):
    part = exchange(packed.reshape(lax.axis_size(SLICED), -1, LANES), SLICED)
    part = whole_sum(part)
    part = exchange(copies(part, WHOLE), WHOLE)
    part = whole_sum(part)
    part = exchange(copies(part, SLICED), SLICED)
    return part.reshape(-1, LANES)


def on_device(state_grid, norm_gain, w_qkv, w_proj, bias_table, window_kind, cotangent):
    _, cols_dev, channels = state_grid.shape
    half_lat, half_lon = WIN_LAT // 2, WIN_LON // 2
    lat, lon = lax.axis_index(LAT), lax.axis_index(LON)
    windows = cols_dev // WIN_LON
    joint = lax.optimization_barrier(jnp.concatenate([state_grid, cotangent], axis=2))
    side = joint[half_lat:, :half_lon]
    up = shifted(joint[:half_lat], LAT, -1)
    lats, lons = lax.axis_size(LAT), lax.axis_size(LON)
    before = [(i * lons + j, (i - 1) % lats * lons + (j - 1) % lons) for i in range(lats) for j in range(lons)]
    corner = lax.ppermute(joint[:half_lat, :half_lon], LAT + LON, before)
    side = shifted(side, LON, -1)
    kinds = lax.dynamic_slice(window_kind, (lat, lon * windows), (1, windows))[0]
    last = (lat == lax.axis_size(LAT) - 1).astype(jnp.int32)
    kind_count, heads, extent = bias_table.shape
    table = bias_table.transpose(1, 0, 2).reshape(heads * kind_count, extent)
    gain = norm_gain.reshape(1, -1)
    packed, *kept = attend(kinds, joint, up, side, corner, gain, w_qkv, w_proj, bias_of(table, last[None]))
    both = results(windows, *kept, gain, w_proj)
    moved = shifted(both[:, -half_lon:], LON, 1)
    placed = jnp.concatenate([moved, both[:, :-half_lon]], axis=1)
    lower = shifted(placed[half_lat:], LAT, 1)
    summed = total_of(packed)
    own = jnp.concatenate([lower, placed[:half_lat]], axis=0).astype(f32)
    out_field = (state_grid.astype(f32) + own[:, :, :channels]).astype(bf16)
    d_field = (cotangent.astype(f32) + own[:, :, channels:]).astype(bf16)
    gq, gp, gt, gg = finish(summed, heads * kind_count, extent)
    gt = gt.reshape(heads, kind_count, extent).transpose(1, 0, 2)
    return (out_field, d_field, gq, gp, gt, gg.reshape(-1))


def solution(mesh):
    in_specs = (P(LAT, LON, None), P(), P(), P(), P(), P(), P(LAT, LON, None))
    out_specs = (P(LAT, LON, None), P(LAT, LON, None), P(), P(), P(), P())
    mesh = Mesh(mesh.devices.reshape(PARTS), LAT + LON)
    return jax.shard_map(on_device, mesh=mesh, in_specs=in_specs, out_specs=out_specs, check_vma=False)
```

```python
import functools
import jax
import jax.numpy as jnp
from jax import lax
from jax.experimental import pallas as pl
from jax.experimental.pallas import tpu as pltpu
from jax.sharding import Mesh, PartitionSpec as P

HEADS = 6
WIN_LAT = 6
WIN_LON = 12
HEAD = 32
D = 192
PITCH = 16
TOK = WIN_LAT * PITCH
LANES = 128
SPAN = 256
norm_eps = 1e-05
clip_eps = 1e-06
masked = -1e30
AT_TABLE = 6 * D
AT_GAIN = AT_TABLE + 96
ROWS = 1280
VM_ATTEND = 28
VM_FINISH = 8
VM_BIAS = 10
VM_RESULTS = 8
LAT = ("y_lo", "z_hi", "z_lo")
LON = ("y_hi", "x", "core")
PARTS = (2, 4, 2, 4, 4, 2)
SLICED = ("y_lo", "z_lo", "x", "core")
WHOLE = ("z_hi", "y_hi")
f32 = jnp.float32
bf16 = jnp.bfloat16

NT = (((1,), (1,)), ((), ()))
TN = (((0,), (0,)), ((), ()))


def nt(a, b, **kw):
    return lax.dot_general(a, b, NT, preferred_element_type=f32, **kw)


def tn(a, b, **kw):
    return lax.dot_general(a, b, TN, preferred_element_type=f32, **kw)


def nn(a, b, **kw):
    return jnp.dot(a, b, preferred_element_type=f32, **kw)


def iota(shape, dim):
    return lax.broadcasted_iota(jnp.int32, shape, dim)


def base_pattern():
    p = iota((SPAN, SPAN), 0)
    lane = iota((SPAN, SPAN), 1)
    d = lane // PITCH
    c = lane % PITCH
    hit = (p == (2 * WIN_LAT - 2 - d) * (2 * WIN_LON - 1) - c + WIN_LON - 1) & (c < WIN_LON) & (d < 2 * WIN_LAT - 1)
    return hit.astype(f32)


def bias_kernel(table_ref, last_ref, bias, tab, tilt, span):
    half_lat = WIN_LAT // 2
    kinds = table_ref.shape[0] // HEADS
    tab[...] = jnp.zeros_like(tab)
    tab[:, :table_ref.shape[1]] = table_ref[...]
    for c in range(PITCH):
        moved = tab[...] if c == 0 else pltpu.roll(tab[...], SPAN - c, axis=1)
        for half in range(2):
            tilt[half, pl.ds(c, kinds * HEADS, stride=PITCH), :] = moved[:, half * LANES:(half + 1) * LANES]
    pattern = base_pattern()
    whole = jnp.concatenate([tilt[0], tilt[1]], axis=1)
    parts = []
    for _ in range(3):
        parts.append(whole.astype(bf16))
        whole = whole - parts[-1].astype(f32)
    pattern = pattern.astype(bf16)
    span[...] = nn(jnp.concatenate(parts, axis=1), jnp.concatenate([pattern] * 3, axis=0))
    slot = iota((PITCH, LANES), 1)
    open_slot = (slot % PITCH < WIN_LON) & (slot < TOK)
    split = last_ref[0] > 0

    def spread(n, carry):
        wide = span[pl.ds(pl.multiple_of(n * PITCH, PITCH), PITCH), :]
        for r in range(WIN_LAT):
            off = (WIN_LAT - 1 - r) * PITCH
            part = wide[:, :LANES]
            if off:
                part = pltpu.roll(part, LANES - off, axis=1)
            if off + TOK > LANES:
                part = jnp.where(slot < LANES - off, part, pltpu.roll(wide[:, LANES:], LANES - off, axis=1))
            other = (slot < half_lat * PITCH) if r >= half_lat else (slot >= half_lat * PITCH)
            ok = open_slot & jnp.logical_not(split & other)
            bias[n % kinds, pl.ds(pl.multiple_of((n // kinds) * TOK + r * PITCH, PITCH), PITCH), :] = jnp.where(ok, part, masked)
        return carry

    lax.fori_loop(0, kinds * HEADS, spread, 0, unroll=True)


def bias_of(table, last):
    vm = pl.BlockSpec(memory_space=pltpu.VMEM)
    kh = table.shape[0]
    return pl.pallas_call(
        bias_kernel,
        out_shape=jax.ShapeDtypeStruct((kh // HEADS, HEADS * TOK, LANES), f32),
        in_specs=[vm, pl.BlockSpec(memory_space=pltpu.SMEM)],
        out_specs=vm,
        scratch_shapes=[
            pltpu.VMEM((kh, SPAN), f32), pltpu.VMEM((2, kh * PITCH, LANES), f32), pltpu.VMEM((kh * PITCH, SPAN), f32),
        ],
        cost_estimate=pl.CostEstimate(flops=600_000_000, bytes_accessed=2_500_000, transcendentals=0),
        compiler_params=pltpu.CompilerParams(vmem_limit_bytes=VM_BIAS << 20),
        name="bias",
    )(table, last)


def kernel(windows, kinds, meta_ref, own_ref, up_ref, side_ref, corner_ref, gain_ref, wqkv_ref, wproj_ref, bias,
           grads_ref, mix, dn_ref, un, inv,
           xs, gs, tilt, nm, q_s, k_s, v_s, dm_s, dq_s, dk_s, dv_s, fold):
    half_lat = WIN_LAT // 2
    half_lon = WIN_LON // 2

    pattern = base_pattern()
    fold[...] = jnp.zeros_like(fold)

    xs[...] = jnp.zeros_like(xs)
    gs[...] = jnp.zeros_like(gs)
    for w in range(windows):
        for r in range(WIN_LAT):
            at = w * TOK + r * PITCH
            start = half_lon + w * WIN_LON
            inside = WIN_LON if w < windows - 1 else half_lon
            for dst, lo in ((xs, 0), (gs, D)):
                if r < half_lat:
                    dst[at:at + inside, :] = own_ref[r + half_lat, start:start + inside, lo:lo + D]
                    if inside < WIN_LON:
                        dst[at + inside:at + WIN_LON, :] = side_ref[r, :, lo:lo + D]
                else:
                    dst[at:at + inside, :] = up_ref[r - half_lat, start:start + inside, lo:lo + D]
                    if inside < WIN_LON:
                        dst[at + inside:at + WIN_LON, :] = corner_ref[r - half_lat, :, lo:lo + D]

    gain = gain_ref[...]
    x = xs[...].astype(f32)
    centre = x - jnp.mean(x, axis=-1, keepdims=True)
    inverse = lax.rsqrt(jnp.mean(centre * centre, axis=-1, keepdims=True) + norm_eps)
    unit = centre * inverse
    un[...] = unit
    inv[...] = inverse
    normed = (unit * gain).astype(bf16)
    nm[...] = normed
    wq, wk, wv = (wqkv_ref[:, i * D:(i + 1) * D] for i in range(3))
    q_s[...] = nn(normed, wq).astype(bf16)
    k_s[...] = nn(normed, wk).astype(bf16)
    v_s[...] = nn(normed, wv).astype(bf16)
    dm_s[...] = nt(gs[...], wproj_ref[...]).astype(bf16)

    key_slot = iota((PITCH, LANES), 1)
    scale = HEAD ** (-0.5)
    head_of = iota((TOK, D), 1) // HEAD
    pads = jnp.zeros((LANES - TOK, D), bf16)

    def by_head(a):
        zero = jnp.zeros_like(a)
        return [jnp.where(head_of == h, a, zero) for h in range(HEADS)]

    def window(w):
        rows = pl.ds(w * TOK, TOK)
        kind = meta_ref[w]
        q, k, v, dm = q_s[rows, :], k_s[rows, :], v_s[rows, :], dm_s[rows, :]
        q_heads = jnp.concatenate(by_head(q), axis=0)
        dm_heads = jnp.concatenate(by_head(dm), axis=0)
        k_pad = jnp.concatenate([k, pads], axis=0)
        v_pad = jnp.concatenate([v, pads], axis=0)
        scores = nt(q_heads, k_pad) * scale + bias[kind]
        top = jnp.max(scores, axis=-1, keepdims=True)
        raised = jnp.exp(scores - top)
        probs = raised * (1.0 / jnp.sum(raised, axis=-1, keepdims=True))
        probs_low = probs.astype(bf16)
        d_probs = nt(dm_heads, v_pad)
        d_scores = probs * (d_probs - jnp.sum(probs * d_probs, axis=-1, keepdims=True))
        low = d_scores.astype(bf16)
        side = lambda a: jnp.concatenate([a[h * TOK:(h + 1) * TOK] for h in range(HEADS)], axis=1)
        tall = lambda a: jnp.concatenate([b for part in by_head(a) for b in (part, pads)], axis=0)
        mix[rows, :] = nn(side(probs_low), tall(v)).astype(bf16)
        dq_s[rows, :] = (nn(side(low), tall(k)) * scale).astype(bf16)
        dv_s[rows, :] = tn(probs_low, dm_heads)[:TOK].astype(bf16)
        dk_s[rows, :] = (tn(low, q_heads) * scale)[:TOK].astype(bf16)
        for h in range(HEADS):
            left = right = jnp.zeros((PITCH, LANES), f32)
            for r in range(WIN_LAT):
                off = (WIN_LAT - 1 - r) * PITCH
                part = d_scores[h * TOK + r * PITCH:h * TOK + (r + 1) * PITCH]
                if off:
                    part = pltpu.roll(part, off, axis=1)
                if off + TOK > LANES:
                    over = key_slot < off + TOK - LANES
                    right = right + jnp.where(over, part, 0.0)
                    part = jnp.where(over, 0.0, part)
                left = left + part
            at = pl.ds(pl.multiple_of((h * kinds + kind) * PITCH, PITCH), PITCH)
            fold[at, :LANES] += left
            fold[at, LANES:] += right

    for w in range(windows):
        window(w)

    gp = tn(mix[...], gs[...]).astype(bf16)
    d_normed = nt(dq_s[...], wq) + nt(dk_s[...], wk) + nt(dv_s[...], wv)
    dn_ref[...] = d_normed
    gq = []
    for d in (dq_s, dk_s, dv_s):
        gq.append(tn(nm[...], d[...]).astype(bf16))
    gq = jnp.concatenate(gq, axis=1)
    for b in range(4):
        grads_ref[b * D:(b + 1) * D, :] = gq[:, b * LANES:(b + 1) * LANES]
    grads_ref[4 * D:5 * D, :] = jnp.concatenate([gq[:, 4 * LANES:], gp[:, LANES:]], axis=1)
    grads_ref[5 * D:6 * D, :] = gp[:, :LANES]
    unit = un[...]
    gg = jnp.sum(d_normed * unit, axis=0, keepdims=True)
    gg = jnp.concatenate([gg[:, :LANES], jnp.concatenate([gg[:, LANES:], jnp.zeros((1, SPAN - D), f32)], axis=1), jnp.zeros((ROWS - AT_GAIN - 2, LANES), f32)], axis=0)
    grads_ref[AT_GAIN:, :] = gg.astype(bf16)

    low_pattern = pattern.astype(bf16)
    step = kinds * PITCH
    for h in range(HEADS):
        part = fold[h * step:(h + 1) * step, :]
        high = part.astype(bf16)
        back = nt(jnp.concatenate([high, (part - high.astype(f32)).astype(bf16)], axis=1), jnp.concatenate([low_pattern, low_pattern], axis=1))
        for half in range(2):
            tilt[half, h * step:(h + 1) * step, :] = back[:, half * LANES:(half + 1) * LANES]
    total = None
    for c in range(WIN_LON):
        part = jnp.concatenate([tilt[half, pl.ds(c, kinds * HEADS, stride=PITCH), :] for half in range(2)], axis=1)
        if c:
            part = pltpu.roll(part, c, axis=1)
        total = part if total is None else total + part
    for half in range(2):
        at = AT_TABLE + half * kinds * HEADS
        grads_ref[at:at + kinds * HEADS, :] = total[:, half * LANES:(half + 1) * LANES].astype(bf16)


def results_kernel(windows, mix, dn_ref, un, inv, gain_ref, wproj_ref, both_ref):
    gain = gain_ref[...]
    branch = nn(mix[...], wproj_ref[...]).astype(bf16)
    d_normed = dn_ref[...]
    unit = un[...]
    d_unit = d_normed * gain
    path = inv[...] * (d_unit - jnp.mean(d_unit, axis=-1, keepdims=True) - unit * jnp.mean(d_unit * unit, axis=-1, keepdims=True))
    path = path.astype(bf16)
    for w in range(windows):
        for r in range(WIN_LAT):
            at = w * TOK + r * PITCH
            both_ref[r, w * WIN_LON:(w + 1) * WIN_LON, 0:D] = branch[at:at + WIN_LON]
            both_ref[r, w * WIN_LON:(w + 1) * WIN_LON, D:2 * D] = path[at:at + WIN_LON]


def results(windows, mix, d_normed, unit, inverse, gain, w_proj):
    vm = pl.BlockSpec(memory_space=pltpu.VMEM)
    return pl.pallas_call(
        functools.partial(results_kernel, windows),
        out_shape=jax.ShapeDtypeStruct((WIN_LAT, windows * WIN_LON, 2 * D), bf16),
        in_specs=[vm] * 6,
        out_specs=vm,
        cost_estimate=pl.CostEstimate(flops=60_000_000, bytes_accessed=2_000_000, transcendentals=0),
        compiler_params=pltpu.CompilerParams(vmem_limit_bytes=VM_RESULTS << 20),
        name="results",
    )(mix, d_normed, unit, inverse, gain, w_proj)


def attend(kinds, own, up, side, corner, gain, w_qkv, w_proj, bias):
    windows = own.shape[1] // WIN_LON
    n = windows * TOK
    vm = pl.BlockSpec(memory_space=pltpu.VMEM)
    kh = bias.shape[0] * HEADS
    return pl.pallas_call(
        functools.partial(kernel, windows, bias.shape[0]),
        out_shape=(
            jax.ShapeDtypeStruct((ROWS, LANES), bf16),
            jax.ShapeDtypeStruct((n, D), bf16),
            jax.ShapeDtypeStruct((n, D), f32),
            jax.ShapeDtypeStruct((n, D), f32),
            jax.ShapeDtypeStruct((n, 1), f32),
        ),
        in_specs=[pl.BlockSpec(memory_space=pltpu.SMEM)] + [vm] * 8,
        out_specs=(vm,) * 5,
        scratch_shapes=[
            pltpu.VMEM((n, D), bf16), pltpu.VMEM((n, D), bf16), pltpu.VMEM((2, kh * PITCH, LANES), f32),
            pltpu.VMEM((n, D), bf16),
        ] + [pltpu.VMEM((n, D), bf16)] * 7 + [pltpu.VMEM((kh * PITCH, SPAN), f32)],
        cost_estimate=pl.CostEstimate(flops=2_000_000_000, bytes_accessed=4_000_000, transcendentals=500_000),
        compiler_params=pltpu.CompilerParams(vmem_limit_bytes=VM_ATTEND << 20),
        name="attend",
    )(kinds, own, up, side, corner, gain, w_qkv, w_proj, bias)


def finish_kernel(grads_ref, gq_ref, gp_ref, gt_ref, gg_ref):
    def scale_of(parts, count):
        total = sum(jnp.sum(jnp.sum(p * p, axis=0, keepdims=True), axis=1, keepdims=True) for p in parts)
        return jnp.minimum(1.0, lax.rsqrt(total / count + clip_eps))

    kh = gt_ref.shape[0]
    wide = [grads_ref[b * D:(b + 1) * D, :].astype(f32) for b in range(4)]
    shared = grads_ref[4 * D:5 * D, :].astype(f32)
    low, high = shared[:, :LANES // 2], shared[:, LANES // 2:]
    first = grads_ref[5 * D:6 * D, :].astype(f32)
    by = scale_of(wide + [low], gq_ref.shape[0] * gq_ref.shape[1])
    for b in range(4):
        gq_ref[:, b * LANES:(b + 1) * LANES] = wide[b] * by
    gq_ref[:, 4 * LANES:] = low * by
    by = scale_of([first, high], gp_ref.shape[0] * gp_ref.shape[1])
    gp_ref[:, :LANES] = first * by
    gp_ref[:, LANES:] = high * by
    left = grads_ref[AT_TABLE:AT_TABLE + kh, :].astype(f32)
    right = grads_ref[AT_TABLE + kh:AT_TABLE + 2 * kh, :].astype(f32)
    by = scale_of([left, right], kh * gt_ref.shape[1])
    gt_ref[:, :LANES] = left * by
    gt_ref[:, LANES:] = (right * by)[:, :gt_ref.shape[1] - LANES]
    rows = grads_ref[AT_GAIN:AT_GAIN + 16, :].astype(f32)
    by = scale_of([rows], D)
    gg_ref[:, :LANES] = rows[0:1] * by
    gg_ref[:, LANES:] = (rows[1:2] * by)[:, :D - LANES]


def finish(grads, table_rows, extent):
    vm = pl.BlockSpec(memory_space=pltpu.VMEM)
    return pl.pallas_call(
        finish_kernel,
        out_shape=(
            jax.ShapeDtypeStruct((D, 3 * D), f32),
            jax.ShapeDtypeStruct((D, D), f32),
            jax.ShapeDtypeStruct((table_rows, extent), f32),
            jax.ShapeDtypeStruct((1, D), f32),
        ),
        in_specs=[vm],
        out_specs=(vm,) * 4,
        cost_estimate=pl.CostEstimate(flops=1_000_000, bytes_accessed=1_000_000, transcendentals=4),
        compiler_params=pltpu.CompilerParams(vmem_limit_bytes=VM_FINISH << 20),
        name="finish",
    )(grads)


def shifted(value, axis, steps):
    count = lax.axis_size(axis)
    return lax.ppermute(value, axis, [(i, (i + steps) % count) for i in range(count)])


def exchange(part, axes):
    return lax.all_to_all(part, axes, 0, 0, tiled=True)


def whole_sum(got):
    return jnp.sum(got.astype(f32), axis=0).astype(bf16)


def copies(part, axes):
    return jnp.broadcast_to(part[None], (lax.axis_size(axes),) + part.shape)


def total_of(packed):
    part = exchange(packed.reshape(lax.axis_size(SLICED), -1, LANES), SLICED)
    part = whole_sum(part)
    part = exchange(copies(part, WHOLE), WHOLE)
    part = whole_sum(part)
    part = exchange(copies(part, SLICED), SLICED)
    return part.reshape(-1, LANES)


def on_device(state_grid, norm_gain, w_qkv, w_proj, bias_table, window_kind, cotangent):
    _, cols_dev, channels = state_grid.shape
    half_lat, half_lon = WIN_LAT // 2, WIN_LON // 2
    lat, lon = lax.axis_index(LAT), lax.axis_index(LON)
    windows = cols_dev // WIN_LON
    joint = lax.optimization_barrier(jnp.concatenate([state_grid, cotangent], axis=2))
    side = joint[half_lat:, :half_lon]
    up = shifted(joint[:half_lat], LAT, -1)
    lats, lons = lax.axis_size(LAT), lax.axis_size(LON)
    before = [(i * lons + j, (i - 1) % lats * lons + (j - 1) % lons) for i in range(lats) for j in range(lons)]
    corner = lax.ppermute(joint[:half_lat, :half_lon], LAT + LON, before)
    side = shifted(side, LON, -1)
    kinds = lax.dynamic_slice(window_kind, (lat, lon * windows), (1, windows))[0]
    last = (lat == lax.axis_size(LAT) - 1).astype(jnp.int32)
    kind_count, heads, extent = bias_table.shape
    table = bias_table.transpose(1, 0, 2).reshape(heads * kind_count, extent)
    gain = norm_gain.reshape(1, -1)
    packed, *kept = attend(kinds, joint, up, side, corner, gain, w_qkv, w_proj, bias_of(table, last[None]))
    both = results(windows, *kept, gain, w_proj)
    moved = shifted(both[:, -half_lon:], LON, 1)
    placed = jnp.concatenate([moved, both[:, :-half_lon]], axis=1)
    lower = shifted(placed[half_lat:], LAT, 1)
    summed = total_of(packed)
    own = jnp.concatenate([lower, placed[:half_lat]], axis=0).astype(f32)
    out_field = (state_grid.astype(f32) + own[:, :, :channels]).astype(bf16)
    d_field = (cotangent.astype(f32) + own[:, :, channels:]).astype(bf16)
    gq, gp, gt, gg = finish(summed, heads * kind_count, extent)
    gt = gt.reshape(heads, kind_count, extent).transpose(1, 0, 2)
    return (out_field, d_field, gq, gp, gt, gg.reshape(-1))


def solution(mesh):
    in_specs = (P(LAT, LON, None), P(), P(), P(), P(), P(), P(LAT, LON, None))
    out_specs = (P(LAT, LON, None), P(LAT, LON, None), P(), P(), P(), P())
    mesh = Mesh(mesh.devices.reshape(PARTS), LAT + LON)
    return jax.shard_map(on_device, mesh=mesh, in_specs=in_specs, out_specs=out_specs, check_vma=False)
```
